32 devices in a mesh: dp: 8 (over y, x, core), tensor: 4 (over z).
Axes of the slice: x: 2, y: 2, z: 4, core: 2. Of those that a mesh axis runs over, the one named last changes fastest.
Arguments:
- grad_tokens: bfloat16 [1536, 2048], P('dp', 'tensor'), may hold values from -6 to 6
- hidden_input: bfloat16 [2048, 5120], P('dp', 'tensor'), may hold values from -6 to 6
- output_weight: bfloat16 [5120, 2048], P(None, 'tensor'), may hold values from -0.078125 to 0.078125
- image_tokens: int32 [8, 8], replicated, may hold values from 0 to 192, as said below
- moved_images: int32 [8], replicated, may hold values from 0 to 7, as said below
Outputs:
- input_grad: bfloat16 [2048, 5120], P('dp', 'tensor')
- weight_grad: float32 [5120, 2048], P('dp', 'tensor')
- bias_grad: float32 [2048], P('tensor')
The draws below stay inside these ranges and needn't reach their ends.
Inputs may be any that keep to these rules, and one draw needn't show every extreme that they name: `image_tokens`: row s lists the merged tokens of sample s's images in order: 1 to 8 positive entries, then zeros; each row sums to 192. `moved_images`: entry s is less than the number of images of sample s; those trailing images hold at most 64 merged tokens together, exactly 64 for some sample in every draw. They are encoded by owner s + 1 (owner 0 after the last).
All inputs are finite; a program needn't handle non-finite values.
Results may differ from the reference program's by a relative error of at most 0.014.
Values may be sent and summed in bfloat16 or wider, within the bound.
A program may use at most 64 MiB of HBM per device.

```python
import jax
import jax.numpy as jnp
from jax import lax

HID = 5120
OUT = 2048
IMAGES = 8
TOK_DEV = 192
MOVE_CAP = 64
ROWS = 256
SAMPLES = 8
TOKENS = 1536
BUF = 2048
HPAD = 5120
N_TENSOR = 4


def plan_images(key):
    base = jax.random.fold_in(key, 1234)
    key_count, key_cut, key_high, key_move, key_pick = jax.random.split(base, 5)
    count_images = jax.random.randint(key_count, (SAMPLES,), 1, IMAGES + 1)
    picked = jax.random.randint(key_pick, (), 0, SAMPLES)
    sample_ids = jnp.arange(SAMPLES)
    single = sample_ids == picked
    chosen = sample_ids == (picked + 1) % SAMPLES
    count_images = jnp.where(single, 1, count_images)
    count_images = jnp.where(chosen, IMAGES, count_images)
    free_cuts = jax.vmap(lambda subkey: jax.random.permutation(subkey, TOK_DEV - 1)[:IMAGES - 1] + 1)(jax.random.split(key_cut, SAMPLES))
    high_cuts = jax.random.permutation(key_high, MOVE_CAP - 1)[:IMAGES - 2] + 1 + TOK_DEV - MOVE_CAP
    chosen_cuts = jnp.concatenate([jnp.full((1,), TOK_DEV - MOVE_CAP, high_cuts.dtype), high_cuts])
    slot_ids = jnp.arange(IMAGES - 1)[None, :]
    cuts = jnp.where(chosen[:, None], chosen_cuts[None, :], free_cuts)
    cuts = jnp.where(slot_ids < count_images[:, None] - 1, cuts, TOK_DEV)
    cuts = jnp.sort(cuts, axis=1).astype(jnp.int32)
    bounds = jnp.concatenate([jnp.zeros((SAMPLES, 1), jnp.int32), cuts, jnp.full((SAMPLES, 1), TOK_DEV, jnp.int32)], axis=1)
    sizes = bounds[:, 1:] - bounds[:, :-1]
    trailing = jnp.arange(IMAGES)[None, :]
    start_index = jnp.clip(count_images[:, None] - trailing, 0, IMAGES)
    starts = jnp.take_along_axis(bounds, start_index, axis=1)
    fitting = (TOK_DEV - starts <= MOVE_CAP) & (trailing < count_images[:, None])
    wanted = jax.random.randint(key_move, (SAMPLES,), 0, IMAGES)
    allowed = fitting & (trailing <= wanted[:, None])
    moved = jnp.max(jnp.where(allowed, trailing, 0), axis=1)
    moved = jnp.where(chosen, IMAGES - 1, moved)
    return (sizes.astype(jnp.int32), moved.astype(jnp.int32))


def draw_image_tokens(key, part):
    return plan_images(key)[0]


def draw_moved_images(key, part):
    return plan_images(key)[1]


def raised(drawn, own_key, source, target, shards_of, factor):
    owner, partner = [(jnp.arange(drawn.shape[axis_at]) // (drawn.shape[axis_at] // shards_of)).reshape([-1 if axis == axis_at else 1 for axis in range(drawn.ndim)]) for axis_at in (source, target)]
    chosen = jax.random.permutation(own_key, shards_of)[partner]
    strong = (owner == chosen) | (owner == (partner + shards_of // 2) % shards_of)
    return jnp.where(strong, factor * drawn, drawn)


def block_scale(rng, extent, cuts, least, high):
    level, own = 1.0, jax.random.fold_in(rng, 6)
    for dim, blocks in cuts:
        heights = jnp.exp(jax.random.uniform(jax.random.fold_in(own, dim), (blocks,), jnp.float32, least / len(cuts), high / len(cuts)))
        level = level * jnp.repeat(heights, extent[dim] // blocks).reshape([-1 if axis == dim else 1 for axis in range(len(extent))])
    return level


def bell_draw(rng, shape, spread, bound, shards=(), kind=jnp.bfloat16):
    result = spread * jax.random.normal(rng, shape, jnp.float32)
    if shards:
        result = result * block_scale(rng, shape, shards, -0.22, 0.18)
    return jnp.clip(result, -bound, bound).astype(kind)


def gaussian_with(own_key, dims, scale, limit, pieces, heavy, held_as=jnp.bfloat16):
    entries = scale * jax.random.normal(own_key, dims, jnp.float32)
    if pieces:
        entries = entries * block_scale(own_key, dims, pieces, -0.22, 0.18)
    return jnp.clip(raised(entries, jax.random.fold_in(own_key, 3), *heavy), -limit, limit).astype(held_as)


def setup_inputs(seed: int = 0) -> dict:
    keys = jax.random.split(jax.random.key(seed), 6)
    grad_tokens = bell_draw(keys[0], (TOKENS, OUT), 1.0, 6.0, ((0, 8), (1, 4)))
    hidden_input = gaussian_with(keys[1], (BUF, HID), 1.0, 6.0, ((0, 8), (1, 4)), (0, 1, 8, 2.0))
    output_weight = bell_draw(keys[2], (HID, OUT), HID ** -0.5, 0.078125, ((1, 4),))
    image_tokens = draw_image_tokens(jax.random.fold_in(keys[5], 71), 0)
    moved_images = draw_moved_images(jax.random.fold_in(keys[5], 71), 0)
    return {"grad_tokens": grad_tokens, "hidden_input": hidden_input, "output_weight": output_weight, "image_tokens": image_tokens, "moved_images": moved_images}


root_half = 0.7071067811865476
inv_root_tau = 0.3989422804014327


def gelu_parts(values):
    normal_cdf = 0.5 * (1.0 + jax.scipy.special.erf(values * root_half))
    density = jnp.exp(-0.5 * values * values) * inv_root_tau
    return values * normal_cdf, normal_cdf + values * density


def kept_lengths(image_tokens, moved_images):
    present = jnp.sum((image_tokens > 0).astype(jnp.int32), axis=1)
    slot_ids = jnp.arange(image_tokens.shape[1], dtype=jnp.int32)
    kept_mask = slot_ids[None, :] < (present - moved_images)[:, None]
    return jnp.sum(jnp.where(kept_mask, image_tokens, 0), axis=1).astype(jnp.int32)


def reference(grad_tokens, hidden_input, output_weight, image_tokens, moved_images):
    keep_len = kept_lengths(image_tokens, moved_images)
    grad_blocks = grad_tokens.reshape(SAMPLES, TOK_DEV, OUT)
    positions = jnp.arange(TOK_DEV, dtype=jnp.int32)
    zero_value = jnp.zeros((), jnp.bfloat16)
    kept_rows = jnp.where(positions[None, :, None] < keep_len[:, None, None], grad_blocks, zero_value)
    moving = jnp.where(positions[None, TOK_DEV - MOVE_CAP:, None] >= keep_len[:, None, None],
                       grad_blocks[:, TOK_DEV - MOVE_CAP:], zero_value)
    buffers = jnp.concatenate([kept_rows, jnp.roll(moving, 1, axis=0)], axis=1)
    bias_grad = jnp.sum(grad_tokens.astype(jnp.float32), axis=0)
    inputs = hidden_input.reshape(SAMPLES, ROWS, HID)
    column_width = OUT // N_TENSOR

    def one_owner(running, owner_data):
        grad_rows, input_rows = owner_data
        grad_hidden = jnp.zeros((ROWS, HID), jnp.float32)
        for tensor_block in range(N_TENSOR):
            low = tensor_block * column_width
            partial_value = lax.dot_general(grad_rows[:, low:low + column_width], output_weight[:, low:low + column_width],
                                      (((1,), (1,)), ((), ())), preferred_element_type=jnp.float32)
            rounded = lax.optimization_barrier(partial_value.astype(jnp.bfloat16))
            grad_hidden = grad_hidden + rounded.astype(jnp.float32)
        activation, slopes = gelu_parts(input_rows.astype(jnp.float32))
        activation = activation.astype(jnp.bfloat16)
        input_grad = (grad_hidden * slopes).astype(jnp.bfloat16)
        running = running + lax.dot_general(activation, grad_rows, (((0,), (0,)), ((), ())),
                                            preferred_element_type=jnp.float32)
        return running, input_grad

    weight_sum, input_grads = lax.scan(one_owner, jnp.zeros((HID, OUT), jnp.float32), (buffers, inputs))
    weight_grad = jnp.concatenate([weight_sum, jnp.zeros((HPAD - HID, OUT), jnp.float32)], axis=0)
    return input_grads.reshape(BUF, HID), weight_grad, bias_grad
```

```python
import functools

import jax
import jax.numpy as jnp
from jax import lax
from jax.experimental import pallas as pl
from jax.experimental.pallas import tpu as pltpu
from jax.sharding import PartitionSpec as P

root_half = 0.7071067811865476
inv_root_tau = 0.3989422804014327
MESH = pl.DeviceIdType.MESH
F32 = jnp.float32
BF16 = jnp.bfloat16


def from_behind(value, axis, steps):
    count = lax.axis_size(axis)
    pairs = [(source, (source + steps) % count) for source in range(count)]
    return lax.ppermute(value, axis, pairs)


def gelu_parts(values):
    normal_cdf = 0.5 * (1.0 + lax.erf(values * root_half))
    density = jnp.exp(-0.5 * values * values) * inv_root_tau
    return (values * normal_cdf, normal_cdf + values * density)


def kept_lengths(image_tokens, moved_images):
    present = jnp.sum((image_tokens > 0).astype(jnp.int32), axis=1)
    slot_ids = jnp.arange(image_tokens.shape[1], dtype=jnp.int32)
    kept_mask = slot_ids[None, :] < (present - moved_images)[:, None]
    return jnp.sum(jnp.where(kept_mask, image_tokens, 0), axis=1)


def per_device_any(grad_tokens, hidden_input, output_weight, image_tokens, moved_images):
    dp_count = lax.axis_size("dp")
    dp_index = lax.axis_index("dp")
    tok_rows = grad_tokens.shape[0]
    buffer_rows = hidden_input.shape[0]
    tail_count = buffer_rows - tok_rows
    keep_len = kept_lengths(image_tokens, moved_images)
    own_keep = jnp.sum(jnp.where(jnp.arange(dp_count, dtype=jnp.int32) == dp_index, keep_len, 0))
    positions = jnp.arange(tok_rows, dtype=jnp.int32)[:, None]
    zero_value = jnp.zeros((), BF16)
    kept_rows = jnp.where(positions < own_keep, grad_tokens, zero_value)
    moving = jnp.where(
        positions[tok_rows - tail_count :] >= own_keep,
        grad_tokens[tok_rows - tail_count :],
        zero_value,
    )
    arrived = from_behind(moving, "dp", 1)
    grad_rows = jnp.concatenate([kept_rows, arrived], axis=0)
    bias_grad = lax.psum(jnp.sum(grad_tokens.astype(F32), axis=0), "dp")
    activation, slopes = gelu_parts(hidden_input.astype(F32))
    partials = lax.dot_general(
        grad_rows, output_weight, (((1,), (1,)), ((), ())), preferred_element_type=F32
    )
    grad_hidden = lax.psum_scatter(
        partials.astype(BF16), "tensor", scatter_dimension=1, tiled=True
    ).astype(F32)
    input_grad = (grad_hidden * slopes).astype(BF16)
    full_act = lax.all_gather(activation.astype(BF16), "tensor", axis=1, tiled=True)
    hidden_width = full_act.shape[1]
    rows_each = (hidden_width + 8 * dp_count - 1) // (8 * dp_count) * 8
    padded = jnp.pad(full_act, ((0, 0), (0, rows_each * dp_count - hidden_width)))
    weight_grad = lax.psum_scatter(
        lax.dot_general(
            padded, grad_rows, (((0,), (0,)), ((), ())), preferred_element_type=F32
        ),
        "dp",
        scatter_dimension=0,
        tiled=True,
    )
    return (input_grad, weight_grad, bias_grad)


def kernel(
    n, dpn,
    g_hbm, x_hbm, w_hbm, it_hbm, mv_hbm,
    xg_ref, wg_ref, bg_ref,
    it_ref, mv_ref, w_ref, x_ref, xn, graw, act, act_other, slope, part, sbuf, up_in, dn_in, wsend, wrecv, wmid, bias,
    tsend, trecv,
    plan_sem, w_sem, x_sem, g_sem, core_s, core_r, act_s, act_r, xt_s, xt_r, tail_s, tail_r,
    up0_s, up0_r, dn0_s, dn0_r, up_s, up_r, dn_s, dn_r, pl_s, pl_r, mid_r, bi_s, bi_r,
):
    dp = lax.axis_index("dp")
    z = lax.axis_index("tensor")
    core = lax.rem(dp, 2)
    chip = lax.div(dp, 2)
    partner = dp + 1 - 2 * core
    after = lax.rem(dp + 1, dpn)
    before = lax.rem(dp + dpn - 1, dpn)
    chips = dpn // 2
    tok = g_hbm.shape[0]
    rows, width = x_hbm.shape
    half = width // 2
    tails = rows - tok
    main = tok - tails
    lane = 128
    nk = half // lane
    ptile = width // nk
    late = 2
    early = range(late, nk)
    main_rows = pl.ds(0, main)
    tail_rows = pl.ds(main, tails)
    slot_rows = pl.ds(tok, tails)

    x_copies = [
        pltpu.make_async_copy(x_hbm.at[slot_rows], x_ref.at[slot_rows], x_sem.at[0]),
        pltpu.make_async_copy(x_hbm.at[pl.ds(0, tok)], x_ref.at[pl.ds(0, tok)], x_sem.at[1]),
    ]
    g_copy = pltpu.make_async_copy(g_hbm, graw.at[core], g_sem)
    w_copy = pltpu.make_async_copy(w_hbm, w_ref, w_sem)
    plan_copies = [
        pltpu.make_async_copy(it_hbm, it_ref, plan_sem.at[0]),
        pltpu.make_async_copy(mv_hbm, mv_ref, plan_sem.at[1]),
    ]
    for c in x_copies + plan_copies:
        c.start()
    g_copy.start()
    w_copy.start()

    barrier = pltpu.get_barrier_semaphore()

    def greet(d, t):
        pl.semaphore_signal(barrier, inc=1, device_id=(d, t), device_id_type=MESH)

    for k in range(1, dpn):
        greet(lax.rem(dp + k, dpn), z)

    @pl.when(z > 0)
    def _():
        greet(dp, z - 1)
        greet(partner, z - 1)

    @pl.when(z < n - 1)
    def _():
        greet(dp, z + 1)
        greet(partner, z + 1)

    pl.semaphore_wait(barrier, dpn - 1 + jnp.where(z > 0, 2, 0) + jnp.where(z < n - 1, 2, 0))

    def remote(src, dst, ss, rs, d, t):
        return pltpu.make_async_remote_copy(
            src_ref=src, dst_ref=dst, send_sem=ss, recv_sem=rs, device_id=(d, t), device_id_type=MESH
        )

    x_tail_copy = remote(x_ref.at[slot_rows], xn, xt_s, xt_r, before, z)
    raw_copy = remote(graw.at[core], graw.at[core], core_s, core_r, partner, z)
    x_copies[0].wait()
    x_tail_copy.start()

    for c in plan_copies:
        c.wait()
    images = it_ref[pl.ds(dp, 1), :].astype(F32)
    present = jnp.sum(jnp.where(images > 0, 1.0, 0.0), axis=1, keepdims=True)
    ids = lax.broadcasted_iota(jnp.int32, images.shape, 1).astype(F32)
    keep = jnp.sum(
        jnp.where(ids < present - mv_ref[dp].astype(F32), images, 0.0), axis=1, keepdims=True
    )

    def stays(columns):
        return lax.broadcasted_iota(jnp.int32, (tails, columns), 0).astype(F32) + main < keep

    def pieces(k):
        if k < late:
            return [(k, 0, tok)]
        return [(k, 0, main), (nk + k - late, main, tails)]

    def act_copy(k, p, r0, rn):
        rs = pl.ds(r0, rn)
        return remote(act_other.at[k, rs], act.at[z, k, core, rs], act_s.at[p], act_r.at[p], partner, z)

    def first_copies(k, p, r0, rn, ss, rr, t):
        rs = pl.ds(r0, rn)
        target = act.at[z, k, core, rs]
        return (
            remote(target, target, ss.at[p, 0], rr.at[p, core], dp, t),
            remote(act_other.at[k, rs], target, ss.at[p, 1], rr.at[p, core], partner, t),
        )

    def send_first(k, p, r0, rn):
        @pl.when(z < n - 1)
        def _():
            for c in first_copies(k, p, r0, rn, up0_s, up0_r, z + 1):
                c.start()

        @pl.when(z > 0)
        def _():
            for c in first_copies(k, p, r0, rn, dn0_s, dn0_r, z - 1):
                c.start()

        act_copy(k, p, r0, rn).start()

    step_rows = 64

    def put(to_other, k, rs, a):
        if to_other:
            act_other[k, rs, :] = a
        else:
            act[z, k, core, rs, :] = a

    def normal_cdf(v):
        return 0.5 * (1.0 + lax.erf(v * root_half))

    def columns_of(which, k):
        return pl.ds(pl.multiple_of(which * half + k * lane, lane), lane)

    def gelu_main(k):
        for which, to_other in ((1 - core, True), (core, False)):
            cols = columns_of(which, k)

            def body(i, carry):
                rs = pl.ds(pl.multiple_of(i * step_rows, step_rows), step_rows)
                v = x_ref[rs, cols].astype(F32)
                cdf = normal_cdf(v)
                slope[rs, cols] = cdf
                put(to_other, k, rs, (v * cdf).astype(BF16))
                return carry

            lax.fori_loop(0, main // step_rows, body, 0)

    def gelu_tail(k):
        for which, to_other in ((1 - core, True), (core, False)):
            cols = columns_of(which, k)
            v = x_ref[tail_rows, cols].astype(F32)
            own = normal_cdf(v)
            slope[tail_rows, cols] = own
            u = xn[:, cols].astype(F32)
            other = normal_cdf(u)
            slope[slot_rows, cols] = other
            put(to_other, k, tail_rows, jnp.where(stays(lane), v * own, u * other).astype(BF16))

    x_copies[1].wait()
    for k in early:
        gelu_main(k)
        send_first(k, *pieces(k)[0])
    g_copy.wait()
    raw_copy.start()
    for k in range(late):
        gelu_main(k)
    x_tail_copy.wait_recv()
    for k in range(nk):
        gelu_tail(k)
        send_first(k, *pieces(k)[-1])

    def up_ag(h, k, r):
        return remote(act.at[h, k], act.at[h, k], up_s.at[r - 1, k], up_r.at[r - 1, k], dp, z + 1)

    def dn_ag(h, k, r):
        return remote(act.at[h, k], act.at[h, k], dn_s.at[r - 1, k], dn_r.at[r - 1, k], dp, z - 1)

    def rs_piece(ref, h, c):
        return ref.at[h, :, tail_rows] if c == 0 else ref.at[h, c - 1, main_rows]

    def up_rs(h, c, r):
        return remote(
            rs_piece(sbuf, h, c), rs_piece(up_in, h, c), up_s.at[r - 1, c], up_r.at[r - 1, c], dp, z + 1
        )

    def dn_rs(h, c, r):
        return remote(
            rs_piece(sbuf, h, c), rs_piece(dn_in, h, c), dn_s.at[r - 1, c], dn_r.at[r - 1, c], dp, z - 1
        )

    def add_up(h, c, extra):
        if c == 0:
            total = part[h, :, main:tok, :]
            if extra is not None:
                total = total + extra[h, :, main:tok, :].astype(F32)
            sbuf[h, :, main:tok, :] = total.astype(BF16)
        else:
            total = part[h, c - 1, 0:main, :]
            if extra is not None:
                total = total + extra[h, c - 1, 0:main, :].astype(F32)
            sbuf[h, c - 1, 0:main, :] = total.astype(BF16)

    w_copy.wait()

    def all_h(i, carry):
        h = lax.div(i, nk)
        k = lax.rem(i, nk)
        at = pl.ds(pl.multiple_of(i * ptile, ptile), ptile)
        part[h, k] = lax.dot_general(
            graw[core], w_ref[at, :], (((1,), (1,)), ((), ())), preferred_element_type=F32
        )
        return carry

    lax.fori_loop(0, n * nk, all_h, 0)

    @pl.when(z == 0)
    def _():
        for r in range(1, n):
            for c in range(nk + 1):
                add_up(n - r, c, None)
                up_rs(n - r, c, r).start()

    @pl.when(z == n - 1)
    def _():
        for r in range(1, n):
            for c in range(nk + 1):
                add_up(r - 1, c, None)
                dn_rs(r - 1, c, r).start()

    raw_copy.wait_recv()
    chip_sum = jnp.sum(graw[0].astype(F32), axis=0, keepdims=True) + jnp.sum(
        graw[1].astype(F32), axis=0, keepdims=True
    )
    bias[chip] = jnp.broadcast_to(chip_sum, bias.shape[1:])

    def bias_copy(k):
        return remote(
            bias.at[chip], bias.at[chip], bi_s.at[k], bi_r.at[chip], lax.rem(dp + 2 * k, dpn), z
        )

    for k in range(1, chips):
        bias_copy(k).start()

    piece = lane // 2

    def relation(h):
        return jnp.where(lax.rem(chip, 2) != lax.rem(h, 2), 1, 0) + jnp.where(
            lax.div(chip, 2) != lax.div(h, 2), 2, 0
        )

    along_x = chip + 1 - 2 * lax.rem(chip, 2)
    along_y = lax.rem(chip + 2, chips)

    def owner_copy(h, k, j):
        role = relation(h) - 1
        return remote(
            wsend.at[h, k, j], wrecv.at[role, k, j], pl_s.at[h, k, j], pl_r.at[role, k, j], h * 2 + core, z
        )

    def corner_copy(h, k, j):
        through = along_x if j == 0 else along_y
        return remote(
            wsend.at[h, k, j], wmid.at[1 - j, k], pl_s.at[h, k, j], mid_r.at[1 - j, k], through * 2 + core, z
        )

    def merge(h, k):
        rel = relation(h)
        for role in (1, 2):
            over = 1 if role == 1 else 0

            @pl.when(rel == role)
            def _():
                corner_copy(h, k, over).wait_recv()
                wsend[h, k, over] = (
                    wsend[h, k, over].astype(F32) + wmid[role - 1, k].astype(F32)
                ).astype(BF16)
                owner_copy(h, k, over).start()

    def weight_tile(h, k):
        acc = lax.dot_general(
            act[h, k].reshape(2 * tok, lane),
            graw[...].reshape(2 * tok, graw.shape[2]),
            (((0,), (0,)), ((), ())),
            preferred_element_type=F32,
        )
        rel = relation(h)

        @pl.when(rel == 0)
        def _():
            wg_ref[k * lane : (k + 1) * lane, :] = acc

        @pl.when(rel != 0)
        def _():
            for j in range(2):
                wsend[h, k, j] = acc[j * piece : (j + 1) * piece].astype(BF16)

        @pl.when(rel == 1)
        def _():
            owner_copy(h, k, 0).start()

        @pl.when(rel == 2)
        def _():
            owner_copy(h, k, 1).start()

        @pl.when(rel == 3)
        def _():
            for j in range(2):
                corner_copy(h, k, j).start()

    for k in range(nk):
        for p, r0, rn in pieces(k):
            act_copy(k, p, r0, rn).wait_recv()
        weight_tile(z, k)

    def merge_round(r, k):
        if r == 0:
            merge(z, k)
        else:

            @pl.when(z >= r)
            def _():
                merge(z - r, k)

            @pl.when(z + r <= n - 1)
            def _():
                merge(z + r, k)

    def first_arrivals(h, k, ss, rr):
        for p, r0, rn in pieces(k):
            rs = pl.ds(r0, rn)
            for s in range(2):
                remote(
                    act.at[h, k, s, rs], act.at[h, k, s, rs], ss.at[p, 0], rr.at[p, s], partner, z
                ).wait_recv()

    def finish_slope(k):
        at = slice(k * ptile, (k + 1) * ptile)

        def grow(source, source_rows, target_rows):
            v = source[source_rows, at].astype(F32)
            slope[target_rows, at] += v * (jnp.exp(-0.5 * v * v) * inv_root_tau)

        def body(i, carry):
            rs = pl.ds(pl.multiple_of(i * step_rows, step_rows), step_rows)
            grow(x_ref, rs, rs)
            return carry

        lax.fori_loop(0, tok // step_rows, body, 0)
        grow(xn, pl.ds(0, tails), slot_rows)

    for r in range(1, n):
        for c in range(nk + 1):
            if c < nk:

                @pl.when(z >= r)
                def _():
                    if r == 1:
                        first_arrivals(z - 1, c, up0_s, up0_r)
                    else:
                        up_ag(z - r, c, r - 1).wait_recv()

                    @pl.when(z < n - 1)
                    def _():
                        up_ag(z - r, c, r).start()

                @pl.when(z + r <= n - 1)
                def _():
                    if r == 1:
                        first_arrivals(z + 1, c, dn0_s, dn0_r)
                    else:
                        dn_ag(z + r, c, r - 1).wait_recv()

                    @pl.when(z > 0)
                    def _():
                        dn_ag(z + r, c, r).start()

            if r > 1:

                @pl.when((z > 0) & (z < r))
                def _():
                    h = n + z - r
                    up_rs(h, c, r - 1).wait_recv()
                    add_up(h, c, up_in)
                    up_rs(h, c, r).start()

                @pl.when((z < n - 1) & (z + r > n - 1))
                def _():
                    h = z + r - n
                    dn_rs(h, c, r - 1).wait_recv()
                    add_up(h, c, dn_in)
                    dn_rs(h, c, r).start()

            if c < nk:

                @pl.when(z >= r)
                def _():
                    weight_tile(z - r, c)

                @pl.when(z + r <= n - 1)
                def _():
                    weight_tile(z + r, c)

                merge_round(r - 1, c)
                if r == 1:
                    finish_slope(c)
                if r == n - 1 and c >= 2:
                    merge_round(r, c - 2)
    for k in range(max(nk - 2, 0), nk):
        merge_round(n - 1, k)

    def last_sum(c):
        index = slice(main, tok) if c == 0 else slice(0, main)
        which = slice(None) if c == 0 else c - 1

        @pl.when(z > 0)
        def _():
            up_rs(z, c, n - 1).wait_recv()
            part[z, which, index, :] += up_in[z, which, index, :].astype(F32)

        @pl.when(z < n - 1)
        def _():
            dn_rs(z, c, n - 1).wait_recv()
            part[z, which, index, :] += dn_in[z, which, index, :].astype(F32)

    last_sum(0)
    zero = jnp.zeros((), F32)
    for k in range(nk):
        at = slice(k * ptile, (k + 1) * ptile)
        total = part[z, k, main:tok, :]
        here = stays(ptile)
        xg_ref[main:tok, at] = jnp.where(here, total * slope[main:tok, at], zero).astype(BF16)
        tsend[:, at] = jnp.where(here, zero, total * slope[tok:rows, at]).astype(BF16)
    tail_copy = remote(tsend, trecv, tail_s, tail_r, after, z)
    tail_copy.start()

    for k in range(1, chips):
        source = lax.rem(chip + k, chips)
        remote(
            bias.at[source], bias.at[source], bi_s.at[k], bi_r.at[source], lax.rem(dp + 2 * k, dpn), z
        ).wait_recv()
    total = bias[0]
    for k in range(1, chips):
        total = total + bias[k]
    bg_ref[...] = total[0]

    for k in range(nk):
        for j in range(2):
            rs = slice(k * lane + j * piece, k * lane + (j + 1) * piece)
            acc = wg_ref[rs, :]
            for role in range(2):
                remote(
                    wsend.at[along_x, k, j], wrecv.at[role, k, j], pl_s.at[0, k, j], pl_r.at[role, k, j],
                    partner, z,
                ).wait_recv()
                acc = acc + wrecv[role, k, j].astype(F32)
            wg_ref[rs, :] = acc

    for k in range(nk):
        last_sum(k + 1)
        at = slice(k * ptile, (k + 1) * ptile)
        xg_ref[0:main, at] = (part[z, k, 0:main, :] * slope[0:main, at]).astype(BF16)

    tail_copy.wait_recv()
    xg_ref[tok:rows, :] = trecv[...]

    tail_copy.wait_send()
    x_tail_copy.wait_send()
    raw_copy.wait_send()
    for c in range(1, chips):
        bias_copy(c).wait_send()
        h = lax.rem(chip + c, chips)
        for k in range(nk):
            for j in range(2):
                remote(
                    wsend.at[h, k, j], wrecv.at[0, k, j], pl_s.at[h, k, j], pl_r.at[0, k, j], partner, z
                ).wait_send()
    for k in range(nk):
        for p in pieces(k):
            act_copy(k, *p).wait_send()

            @pl.when(z < n - 1)
            def _():
                for c in first_copies(k, *p, up0_s, up0_r, z + 1):
                    c.wait_send()

            @pl.when(z > 0)
            def _():
                for c in first_copies(k, *p, dn0_s, dn0_r, z - 1):
                    c.wait_send()

    for r in range(1, n):

        @pl.when((z < n - 1) & (z >= r))
        def _():
            for k in range(nk):
                up_ag(0, k, r).wait_send()

        @pl.when((z < n - 1) & (z < r))
        def _():
            for c in range(nk + 1):
                up_rs(0, c, r).wait_send()

        @pl.when((z > 0) & (z + r <= n - 1))
        def _():
            for k in range(nk):
                dn_ag(0, k, r).wait_send()

        @pl.when((z > 0) & (z + r > n - 1))
        def _():
            for c in range(nk + 1):
                dn_rs(0, c, r).wait_send()


def per_device_fast(n, dpn, grad_tokens, hidden_input, output_weight, image_tokens, moved_images):
    tok, cols = grad_tokens.shape
    rows, width = hidden_input.shape
    half = width // 2
    chips = dpn // 2
    lane = 128
    nk = half // lane
    ptile = width // nk
    npiece = 2 * nk - 2
    dma = pltpu.SemaphoreType.DMA
    vmem = pl.BlockSpec(memory_space=pltpu.VMEM)
    hbm = pl.BlockSpec(memory_space=pltpu.HBM)
    return pl.pallas_call(
        functools.partial(kernel, n, dpn),
        out_shape=(
            jax.ShapeDtypeStruct((rows, width), BF16),
            jax.ShapeDtypeStruct((half, cols), F32),
            jax.ShapeDtypeStruct((cols,), F32),
        ),
        in_specs=[hbm] * 5,
        out_specs=(vmem, vmem, vmem),
        scratch_shapes=[
            pltpu.VMEM(image_tokens.shape, jnp.int32),
            pltpu.SMEM(moved_images.shape, jnp.int32),
            pltpu.VMEM(output_weight.shape, BF16),
            pltpu.VMEM((rows, width), BF16),
            pltpu.VMEM((rows - tok, width), BF16),
            pltpu.VMEM((2, tok, cols), BF16),
            pltpu.VMEM((n, nk, 2, tok, lane), BF16),
            pltpu.VMEM((nk, tok, lane), BF16),
            pltpu.VMEM((rows, width), F32),
            pltpu.VMEM((n, nk, tok, ptile), F32),
            pltpu.VMEM((n, nk, tok, ptile), BF16),
            pltpu.VMEM((n, nk, tok, ptile), BF16),
            pltpu.VMEM((n, nk, tok, ptile), BF16),
            pltpu.VMEM((chips, nk, 2, lane // 2, cols), BF16),
            pltpu.VMEM((2, nk, 2, lane // 2, cols), BF16),
            pltpu.VMEM((2, nk, lane // 2, cols), BF16),
            pltpu.VMEM((chips, 8, cols), F32),
            pltpu.VMEM((rows - tok, width), BF16),
            pltpu.VMEM((rows - tok, width), BF16),
            dma((2,)),
            dma,
            dma((2,)),
            dma,
            dma,
            dma,
            dma((npiece,)),
            dma((npiece,)),
            dma,
            dma,
            dma,
            dma,
            dma((npiece, 2)),
            dma((npiece, 2)),
            dma((npiece, 2)),
            dma((npiece, 2)),
            dma((n - 1, nk + 1)),
            dma((n - 1, nk + 1)),
            dma((n - 1, nk + 1)),
            dma((n - 1, nk + 1)),
            dma((chips, nk, 2)),
            dma((2, nk, 2)),
            dma((2, nk)),
            dma((chips,)),
            dma((chips,)),
        ],
        compiler_params=pltpu.CompilerParams(
            collective_id=0, has_side_effects=True, vmem_limit_bytes=48 * 1024 * 1024
        ),
    )(grad_tokens, hidden_input, output_weight, image_tokens, moved_images)


def solution(mesh):
    n, dpn = mesh.shape["tensor"], mesh.shape["dp"]
    fast = dpn == 2 * n == 2 * 2 * 2
    return jax.shard_map(
        functools.partial(per_device_fast, n, dpn) if fast else per_device_any,
        mesh=mesh,
        in_specs=(P("dp", "tensor"), P("dp", "tensor"), P(None, "tensor"), P(), P()),
        out_specs=(P("dp", "tensor"), P("dp", "tensor"), P("tensor")),
        check_vma=False,
    )
```

```python
import functools

import jax
import jax.numpy as jnp
from jax import lax
from jax.experimental import pallas as pl
from jax.experimental.pallas import tpu as pltpu
from jax.sharding import PartitionSpec as P

root_half = 0.7071067811865476
inv_root_tau = 0.3989422804014327
MESH = pl.DeviceIdType.MESH
F32 = jnp.float32
BF16 = jnp.bfloat16


def from_behind(value, axis, steps):
    count = lax.axis_size(axis)
    pairs = [(source, (source + steps) % count) for source in range(count)]
    return lax.ppermute(value, axis, pairs)


def gelu_parts(values):
    normal_cdf = 0.5 * (1.0 + lax.erf(values * root_half))
    density = jnp.exp(-0.5 * values * values) * inv_root_tau
    return (values * normal_cdf, normal_cdf + values * density)


def kept_lengths(image_tokens, moved_images):
    present = jnp.sum((image_tokens > 0).astype(jnp.int32), axis=1)
    slot_ids = jnp.arange(image_tokens.shape[1], dtype=jnp.int32)
    kept_mask = slot_ids[None, :] < (present - moved_images)[:, None]
    return jnp.sum(jnp.where(kept_mask, image_tokens, 0), axis=1)


def per_device_any(grad_tokens, hidden_input, output_weight, image_tokens, moved_images):
    dp_count = lax.axis_size("dp")
    dp_index = lax.axis_index("dp")
    tok_rows = grad_tokens.shape[0]
    buffer_rows = hidden_input.shape[0]
    tail_count = buffer_rows - tok_rows
    keep_len = kept_lengths(image_tokens, moved_images)
    own_keep = jnp.sum(jnp.where(jnp.arange(dp_count, dtype=jnp.int32) == dp_index, keep_len, 0))
    positions = jnp.arange(tok_rows, dtype=jnp.int32)[:, None]
    zero_value = jnp.zeros((), BF16)
    kept_rows = jnp.where(positions < own_keep, grad_tokens, zero_value)
    moving = jnp.where(
        positions[tok_rows - tail_count :] >= own_keep,
        grad_tokens[tok_rows - tail_count :],
        zero_value,
    )
    arrived = from_behind(moving, "dp", 1)
    grad_rows = jnp.concatenate([kept_rows, arrived], axis=0)
    bias_grad = lax.psum(jnp.sum(grad_tokens.astype(F32), axis=0), "dp")
    activation, slopes = gelu_parts(hidden_input.astype(F32))
    partials = lax.dot_general(
        grad_rows, output_weight, (((1,), (1,)), ((), ())), preferred_element_type=F32
    )
    grad_hidden = lax.psum_scatter(
        partials.astype(BF16), "tensor", scatter_dimension=1, tiled=True
    ).astype(F32)
    input_grad = (grad_hidden * slopes).astype(BF16)
    full_act = lax.all_gather(activation.astype(BF16), "tensor", axis=1, tiled=True)
    hidden_width = full_act.shape[1]
    rows_each = (hidden_width + 8 * dp_count - 1) // (8 * dp_count) * 8
    padded = jnp.pad(full_act, ((0, 0), (0, rows_each * dp_count - hidden_width)))
    weight_grad = lax.psum_scatter(
        lax.dot_general(
            padded, grad_rows, (((0,), (0,)), ((), ())), preferred_element_type=F32
        ),
        "dp",
        scatter_dimension=0,
        tiled=True,
    )
    return (input_grad, weight_grad, bias_grad)


def kernel(
    n, dpn,
    g_hbm, x_hbm, w_hbm, it_hbm, mv_hbm,
    xg_ref, wg_ref, bg_ref,
    it_ref, mv_ref, w_ref, x_ref, xn, graw, act, act_other, slope, part, sbuf, up_in, dn_in, wsend, wrecv, wmid, bias,
    tsend, trecv,
    plan_sem, w_sem, x_sem, g_sem, core_s, core_r, act_s, act_r, xt_s, xt_r, tail_s, tail_r,
    up0_s, up0_r, dn0_s, dn0_r, up_s, up_r, dn_s, dn_r, pl_s, pl_r, mid_r, bi_s, bi_r,
):
    dp = lax.axis_index("dp")
    z = lax.axis_index("tensor")
    core = lax.rem(dp, 2)
    chip = lax.div(dp, 2)
    partner = dp + 1 - 2 * core
    after = lax.rem(dp + 1, dpn)
    before = lax.rem(dp + dpn - 1, dpn)
    chips = dpn // 2
    tok = g_hbm.shape[0]
    rows, width = x_hbm.shape
    half = width // 2
    tails = rows - tok
    main = tok - tails
    lane = 128
    nk = half // lane
    ptile = width // nk
    late = 2
    early = range(late, nk)
    main_rows = pl.ds(0, main)
    tail_rows = pl.ds(main, tails)
    slot_rows = pl.ds(tok, tails)

    x_copies = [
        pltpu.make_async_copy(x_hbm.at[slot_rows], x_ref.at[slot_rows], x_sem.at[0]),
        pltpu.make_async_copy(x_hbm.at[pl.ds(0, tok)], x_ref.at[pl.ds(0, tok)], x_sem.at[1]),
    ]
    g_copy = pltpu.make_async_copy(g_hbm, graw.at[core], g_sem)
    w_copy = pltpu.make_async_copy(w_hbm, w_ref, w_sem)
    plan_copies = [
        pltpu.make_async_copy(it_hbm, it_ref, plan_sem.at[0]),
        pltpu.make_async_copy(mv_hbm, mv_ref, plan_sem.at[1]),
    ]
    for c in x_copies + plan_copies:
        c.start()
    g_copy.start()
    w_copy.start()

    barrier = pltpu.get_barrier_semaphore()

    def greet(d, t):
        pl.semaphore_signal(barrier, inc=1, device_id=(d, t), device_id_type=MESH)

    for k in range(1, dpn):
        greet(lax.rem(dp + k, dpn), z)

    @pl.when(z > 0)
    def _():
        greet(dp, z - 1)
        greet(partner, z - 1)

    @pl.when(z < n - 1)
    def _():
        greet(dp, z + 1)
        greet(partner, z + 1)

    pl.semaphore_wait(barrier, dpn - 1 + jnp.where(z > 0, 2, 0) + jnp.where(z < n - 1, 2, 0))

    def remote(src, dst, ss, rs, d, t):
        return pltpu.make_async_remote_copy(
            src_ref=src, dst_ref=dst, send_sem=ss, recv_sem=rs, device_id=(d, t), device_id_type=MESH
        )

    x_tail_copy = remote(x_ref.at[slot_rows], xn, xt_s, xt_r, before, z)
    raw_copy = remote(graw.at[core], graw.at[core], core_s, core_r, partner, z)
    x_copies[0].wait()
    x_tail_copy.start()

    for c in plan_copies:
        c.wait()
    images = it_ref[pl.ds(dp, 1), :].astype(F32)
    present = jnp.sum(jnp.where(images > 0, 1.0, 0.0), axis=1, keepdims=True)
    ids = lax.broadcasted_iota(jnp.int32, images.shape, 1).astype(F32)
    keep = jnp.sum(
        jnp.where(ids < present - mv_ref[dp].astype(F32), images, 0.0), axis=1, keepdims=True
    )

    def stays(columns):
        return lax.broadcasted_iota(jnp.int32, (tails, columns), 0).astype(F32) + main < keep

    def pieces(k):
        if k < late:
            return [(k, 0, tok)]
        return [(k, 0, main), (nk + k - late, main, tails)]

    def act_copy(k, p, r0, rn):
        rs = pl.ds(r0, rn)
        return remote(act_other.at[k, rs], act.at[z, k, core, rs], act_s.at[p], act_r.at[p], partner, z)

    def first_copies(k, p, r0, rn, ss, rr, t):
        rs = pl.ds(r0, rn)
        target = act.at[z, k, core, rs]
        return (
            remote(target, target, ss.at[p, 0], rr.at[p, core], dp, t),
            remote(act_other.at[k, rs], target, ss.at[p, 1], rr.at[p, core], partner, t),
        )

    def send_first(k, p, r0, rn):
        @pl.when(z < n - 1)
        def _():
            for c in first_copies(k, p, r0, rn, up0_s, up0_r, z + 1):
                c.start()

        @pl.when(z > 0)
        def _():
            for c in first_copies(k, p, r0, rn, dn0_s, dn0_r, z - 1):
                c.start()

        act_copy(k, p, r0, rn).start()

    step_rows = 64

    def put(to_other, k, rs, a):
        if to_other:
            act_other[k, rs, :] = a
        else:
            act[z, k, core, rs, :] = a

    def normal_cdf(v):
        return 0.5 * (1.0 + lax.erf(v * root_half))

    def columns_of(which, k):
        return pl.ds(pl.multiple_of(which * half + k * lane, lane), lane)

    def gelu_main(k):
        for which, to_other in ((1 - core, True), (core, False)):
            cols = columns_of(which, k)

            def body(i, carry):
                rs = pl.ds(pl.multiple_of(i * step_rows, step_rows), step_rows)
                v = x_ref[rs, cols].astype(F32)
                cdf = normal_cdf(v)
                slope[rs, cols] = cdf
                put(to_other, k, rs, (v * cdf).astype(BF16))
                return carry

            lax.fori_loop(0, main // step_rows, body, 0)

    def gelu_tail(k):
        for which, to_other in ((1 - core, True), (core, False)):
            cols = columns_of(which, k)
            v = x_ref[tail_rows, cols].astype(F32)
            own = normal_cdf(v)
            slope[tail_rows, cols] = own
            u = xn[:, cols].astype(F32)
            other = normal_cdf(u)
            slope[slot_rows, cols] = other
            put(to_other, k, tail_rows, jnp.where(stays(lane), v * own, u * other).astype(BF16))

    x_copies[1].wait()
    for k in early:
        gelu_main(k)
        send_first(k, *pieces(k)[0])
    g_copy.wait()
    raw_copy.start()
    for k in range(late):
        gelu_main(k)
    x_tail_copy.wait_recv()
    for k in range(nk):
        gelu_tail(k)
        send_first(k, *pieces(k)[-1])

    def up_ag(h, k, r):
        return remote(act.at[h, k], act.at[h, k], up_s.at[r - 1, k], up_r.at[r - 1, k], dp, z + 1)

    def dn_ag(h, k, r):
        return remote(act.at[h, k], act.at[h, k], dn_s.at[r - 1, k], dn_r.at[r - 1, k], dp, z - 1)

    def rs_piece(ref, h, c):
        return ref.at[h, :, tail_rows] if c == 0 else ref.at[h, c - 1, main_rows]

    def up_rs(h, c, r):
        return remote(
            rs_piece(sbuf, h, c), rs_piece(up_in, h, c), up_s.at[r - 1, c], up_r.at[r - 1, c], dp, z + 1
        )

    def dn_rs(h, c, r):
        return remote(
            rs_piece(sbuf, h, c), rs_piece(dn_in, h, c), dn_s.at[r - 1, c], dn_r.at[r - 1, c], dp, z - 1
        )

    def add_up(h, c, extra):
        if c == 0:
            total = part[h, :, main:tok, :]
            if extra is not None:
                total = total + extra[h, :, main:tok, :].astype(F32)
            sbuf[h, :, main:tok, :] = total.astype(BF16)
        else:
            total = part[h, c - 1, 0:main, :]
            if extra is not None:
                total = total + extra[h, c - 1, 0:main, :].astype(F32)
            sbuf[h, c - 1, 0:main, :] = total.astype(BF16)

    w_copy.wait()

    def all_h(i, carry):
        h = lax.div(i, nk)
        k = lax.rem(i, nk)
        at = pl.ds(pl.multiple_of(i * ptile, ptile), ptile)
        part[h, k] = lax.dot_general(
            graw[core], w_ref[at, :], (((1,), (1,)), ((), ())), preferred_element_type=F32
        )
        return carry

    lax.fori_loop(0, n * nk, all_h, 0)

    @pl.when(z == 0)
    def _():
        for r in range(1, n):
            for c in range(nk + 1):
                add_up(n - r, c, None)
                up_rs(n - r, c, r).start()

    @pl.when(z == n - 1)
    def _():
        for r in range(1, n):
            for c in range(nk + 1):
                add_up(r - 1, c, None)
                dn_rs(r - 1, c, r).start()

    raw_copy.wait_recv()
    chip_sum = jnp.sum(graw[0].astype(F32), axis=0, keepdims=True) + jnp.sum(
        graw[1].astype(F32), axis=0, keepdims=True
    )
    bias[chip] = jnp.broadcast_to(chip_sum, bias.shape[1:])

    def bias_copy(k):
        return remote(
            bias.at[chip], bias.at[chip], bi_s.at[k], bi_r.at[chip], lax.rem(dp + 2 * k, dpn), z
        )

    for k in range(1, chips):
        bias_copy(k).start()

    piece = lane // 2

    def relation(h):
        return jnp.where(lax.rem(chip, 2) != lax.rem(h, 2), 1, 0) + jnp.where(
            lax.div(chip, 2) != lax.div(h, 2), 2, 0
        )

    along_x = chip + 1 - 2 * lax.rem(chip, 2)
    along_y = lax.rem(chip + 2, chips)

    def owner_copy(h, k, j):
        role = relation(h) - 1
        return remote(
            wsend.at[h, k, j], wrecv.at[role, k, j], pl_s.at[h, k, j], pl_r.at[role, k, j], h * 2 + core, z
        )

    def corner_copy(h, k, j):
        through = along_x if j == 0 else along_y
        return remote(
            wsend.at[h, k, j], wmid.at[1 - j, k], pl_s.at[h, k, j], mid_r.at[1 - j, k], through * 2 + core, z
        )

    def merge(h, k):
        rel = relation(h)
        for role in (1, 2):
            over = 1 if role == 1 else 0

            @pl.when(rel == role)
            def _():
                corner_copy(h, k, over).wait_recv()
                wsend[h, k, over] = (
                    wsend[h, k, over].astype(F32) + wmid[role - 1, k].astype(F32)
                ).astype(BF16)
                owner_copy(h, k, over).start()

    def weight_tile(h, k):
        acc = lax.dot_general(
            act[h, k].reshape(2 * tok, lane),
            graw[...].reshape(2 * tok, graw.shape[2]),
            (((0,), (0,)), ((), ())),
            preferred_element_type=F32,
        )
        rel = relation(h)

        @pl.when(rel == 0)
        def _():
            wg_ref[k * lane : (k + 1) * lane, :] = acc

        @pl.when(rel != 0)
        def _():
            for j in range(2):
                wsend[h, k, j] = acc[j * piece : (j + 1) * piece].astype(BF16)

        @pl.when(rel == 1)
        def _():
            owner_copy(h, k, 0).start()

        @pl.when(rel == 2)
        def _():
            owner_copy(h, k, 1).start()

        @pl.when(rel == 3)
        def _():
            for j in range(2):
                corner_copy(h, k, j).start()

    for k in range(nk):
        for p, r0, rn in pieces(k):
            act_copy(k, p, r0, rn).wait_recv()
        weight_tile(z, k)

    def merge_round(r, k):
        if r == 0:
            merge(z, k)
        else:

            @pl.when(z >= r)
            def _():
                merge(z - r, k)

            @pl.when(z + r <= n - 1)
            def _():
                merge(z + r, k)

    def first_arrivals(h, k, ss, rr):
        for p, r0, rn in pieces(k):
            rs = pl.ds(r0, rn)
            for s in range(2):
                remote(
                    act.at[h, k, s, rs], act.at[h, k, s, rs], ss.at[p, 0], rr.at[p, s], partner, z
                ).wait_recv()

    def finish_slope(k):
        at = slice(k * ptile, (k + 1) * ptile)

        def grow(source, source_rows, target_rows):
            v = source[source_rows, at].astype(F32)
            slope[target_rows, at] += v * (jnp.exp(-0.5 * v * v) * inv_root_tau)

        def body(i, carry):
            rs = pl.ds(pl.multiple_of(i * step_rows, step_rows), step_rows)
            grow(x_ref, rs, rs)
            return carry

        lax.fori_loop(0, tok // step_rows, body, 0)
        grow(xn, pl.ds(0, tails), slot_rows)

    for r in range(1, n):
        for c in range(nk + 1):
            if c < nk:

                @pl.when(z >= r)
                def _():
                    if r == 1:
                        first_arrivals(z - 1, c, up0_s, up0_r)
                    else:
                        up_ag(z - r, c, r - 1).wait_recv()

                    @pl.when(z < n - 1)
                    def _():
                        up_ag(z - r, c, r).start()

                @pl.when(z + r <= n - 1)
                def _():
                    if r == 1:
                        first_arrivals(z + 1, c, dn0_s, dn0_r)
                    else:
                        dn_ag(z + r, c, r - 1).wait_recv()

                    @pl.when(z > 0)
                    def _():
                        dn_ag(z + r, c, r).start()

            if r > 1:

                @pl.when((z > 0) & (z < r))
                def _():
                    h = n + z - r
                    up_rs(h, c, r - 1).wait_recv()
                    add_up(h, c, up_in)
                    up_rs(h, c, r).start()

                @pl.when((z < n - 1) & (z + r > n - 1))
                def _():
                    h = z + r - n
                    dn_rs(h, c, r - 1).wait_recv()
                    add_up(h, c, dn_in)
                    dn_rs(h, c, r).start()

            if c < nk:

                @pl.when(z >= r)
                def _():
                    weight_tile(z - r, c)

                @pl.when(z + r <= n - 1)
                def _():
                    weight_tile(z + r, c)

                merge_round(r - 1, c)
                if r == 1:
                    finish_slope(c)
                if r == n - 1 and c >= 2:
                    merge_round(r, c - 2)
    for k in range(max(nk - 2, 0), nk):
        merge_round(n - 1, k)

    def last_sum(c):
        index = slice(main, tok) if c == 0 else slice(0, main)
        which = slice(None) if c == 0 else c - 1

        @pl.when(z > 0)
        def _():
            up_rs(z, c, n - 1).wait_recv()
            part[z, which, index, :] += up_in[z, which, index, :].astype(F32)

        @pl.when(z < n - 1)
        def _():
            dn_rs(z, c, n - 1).wait_recv()
            part[z, which, index, :] += dn_in[z, which, index, :].astype(F32)

    last_sum(0)
    zero = jnp.zeros((), F32)
    for k in range(nk):
        at = slice(k * ptile, (k + 1) * ptile)
        total = part[z, k, main:tok, :]
        here = stays(ptile)
        xg_ref[main:tok, at] = jnp.where(here, total * slope[main:tok, at], zero).astype(BF16)
        tsend[:, at] = jnp.where(here, zero, total * slope[tok:rows, at]).astype(BF16)
    tail_copy = remote(tsend, trecv, tail_s, tail_r, after, z)
    tail_copy.start()

    for k in range(1, chips):
        source = lax.rem(chip + k, chips)
        remote(
            bias.at[source], bias.at[source], bi_s.at[k], bi_r.at[source], lax.rem(dp + 2 * k, dpn), z
        ).wait_recv()
    total = bias[0]
    for k in range(1, chips):
        total = total + bias[k]
    bg_ref[...] = total[0]

    for k in range(nk):
        for j in range(2):
            rs = slice(k * lane + j * piece, k * lane + (j + 1) * piece)
            acc = wg_ref[rs, :]
            for role in range(2):
                remote(
                    wsend.at[along_x, k, j], wrecv.at[role, k, j], pl_s.at[0, k, j], pl_r.at[role, k, j],
                    partner, z,
                ).wait_recv()
                acc = acc + wrecv[role, k, j].astype(F32)
            wg_ref[rs, :] = acc

    for k in range(nk):
        last_sum(k + 1)
        at = slice(k * ptile, (k + 1) * ptile)
        xg_ref[0:main, at] = (part[z, k, 0:main, :] * slope[0:main, at]).astype(BF16)

    tail_copy.wait_recv()
    xg_ref[tok:rows, :] = trecv[...]

    tail_copy.wait_send()
    x_tail_copy.wait_send()
    raw_copy.wait_send()
    for c in range(1, chips):
        bias_copy(c).wait_send()
        h = lax.rem(chip + c, chips)
        for k in range(nk):
            for j in range(2):
                remote(
                    wsend.at[h, k, j], wrecv.at[0, k, j], pl_s.at[h, k, j], pl_r.at[0, k, j], partner, z
                ).wait_send()
    for k in range(nk):
        for p in pieces(k):
            act_copy(k, *p).wait_send()

            @pl.when(z < n - 1)
            def _():
                for c in first_copies(k, *p, up0_s, up0_r, z + 1):
                    c.wait_send()

            @pl.when(z > 0)
            def _():
                for c in first_copies(k, *p, dn0_s, dn0_r, z - 1):
                    c.wait_send()

    for r in range(1, n):

        @pl.when((z < n - 1) & (z >= r))
        def _():
            for k in range(nk):
                up_ag(0, k, r).wait_send()

        @pl.when((z < n - 1) & (z < r))
        def _():
            for c in range(nk + 1):
                up_rs(0, c, r).wait_send()

        @pl.when((z > 0) & (z + r <= n - 1))
        def _():
            for k in range(nk):
                dn_ag(0, k, r).wait_send()

        @pl.when((z > 0) & (z + r > n - 1))
        def _():
            for c in range(nk + 1):
                dn_rs(0, c, r).wait_send()


def writer(a_ref, b_ref, c_ref, a_out, b_out, c_out, sems):
    copies = [
        pltpu.make_async_copy(b_ref, b_out, sems.at[0]),
        pltpu.make_async_copy(a_ref, a_out, sems.at[1]),
        pltpu.make_async_copy(c_ref, c_out, sems.at[2]),
    ]
    for c in copies:
        c.start()
    for c in copies:
        c.wait()


def write_out(*args):
    vmem = pl.BlockSpec(memory_space=pltpu.VMEM)
    hbm = pl.BlockSpec(memory_space=pltpu.HBM)
    return pl.pallas_call(
        writer,
        out_shape=tuple(jax.ShapeDtypeStruct(a.shape, a.dtype) for a in args),
        in_specs=[vmem] * len(args),
        out_specs=tuple([hbm] * len(args)),
        scratch_shapes=[pltpu.SemaphoreType.DMA((len(args),))],
        compiler_params=pltpu.CompilerParams(vmem_limit_bytes=1024 * 1024),
    )(*(pltpu.with_memory_space_constraint(a, pltpu.VMEM) for a in args))


def per_device_fast(n, dpn, *args):
    grad_tokens, hidden_input, output_weight, image_tokens, moved_images = args
    tok, cols = grad_tokens.shape
    rows, width = hidden_input.shape
    half = width // 2
    chips = dpn // 2
    lane = 128
    nk = half // lane
    ptile = width // nk
    npiece = 2 * nk - 2
    dma = pltpu.SemaphoreType.DMA
    vmem = pl.BlockSpec(memory_space=pltpu.VMEM)
    hbm = pl.BlockSpec(memory_space=pltpu.HBM)
    results = pl.pallas_call(
        functools.partial(kernel, n, dpn),
        out_shape=(
            jax.ShapeDtypeStruct((rows, width), BF16),
            jax.ShapeDtypeStruct((half, cols), F32),
            jax.ShapeDtypeStruct((cols,), F32),
        ),
        in_specs=[hbm] * 5,
        out_specs=(vmem, vmem, vmem),
        scratch_shapes=[
            pltpu.VMEM(image_tokens.shape, jnp.int32),
            pltpu.SMEM(moved_images.shape, jnp.int32),
            pltpu.VMEM(output_weight.shape, BF16),
            pltpu.VMEM((rows, width), BF16),
            pltpu.VMEM((rows - tok, width), BF16),
            pltpu.VMEM((2, tok, cols), BF16),
            pltpu.VMEM((n, nk, 2, tok, lane), BF16),
            pltpu.VMEM((nk, tok, lane), BF16),
            pltpu.VMEM((rows, width), F32),
            pltpu.VMEM((n, nk, tok, ptile), F32),
            pltpu.VMEM((n, nk, tok, ptile), BF16),
            pltpu.VMEM((n, nk, tok, ptile), BF16),
            pltpu.VMEM((n, nk, tok, ptile), BF16),
            pltpu.VMEM((chips, nk, 2, lane // 2, cols), BF16),
            pltpu.VMEM((2, nk, 2, lane // 2, cols), BF16),
            pltpu.VMEM((2, nk, lane // 2, cols), BF16),
            pltpu.VMEM((chips, 8, cols), F32),
            pltpu.VMEM((rows - tok, width), BF16),
            pltpu.VMEM((rows - tok, width), BF16),
            dma((2,)),
            dma,
            dma((2,)),
            dma,
            dma,
            dma,
            dma((npiece,)),
            dma((npiece,)),
            dma,
            dma,
            dma,
            dma,
            dma((npiece, 2)),
            dma((npiece, 2)),
            dma((npiece, 2)),
            dma((npiece, 2)),
            dma((n - 1, nk + 1)),
            dma((n - 1, nk + 1)),
            dma((n - 1, nk + 1)),
            dma((n - 1, nk + 1)),
            dma((chips, nk, 2)),
            dma((2, nk, 2)),
            dma((2, nk)),
            dma((chips,)),
            dma((chips,)),
        ],
        compiler_params=pltpu.CompilerParams(
            collective_id=0, has_side_effects=True, vmem_limit_bytes=48 * 1024 * 1024
        ),
    )(*(pltpu.with_memory_space_constraint(a, pltpu.HBM) for a in args))
    return write_out(*results)


def solution(mesh):
    n, dpn = mesh.shape["tensor"], mesh.shape["dp"]
    fast = dpn == 2 * n == 2 * 2 * 2
    return jax.shard_map(
        functools.partial(per_device_fast, n, dpn) if fast else per_device_any,
        mesh=mesh,
        in_specs=(P("dp", "tensor"), P("dp", "tensor"), P(None, "tensor"), P(), P()),
        out_specs=(P("dp", "tensor"), P("dp", "tensor"), P("tensor")),
        check_vma=False,
    )
```

```python
import functools

import jax
import jax.numpy as jnp
from jax import lax
from jax.experimental import pallas as pl
from jax.experimental.pallas import tpu as pltpu
from jax.sharding import PartitionSpec as P

root_half = 0.7071067811865476
inv_root_tau = 0.3989422804014327
MESH = pl.DeviceIdType.MESH
F32 = jnp.float32
BF16 = jnp.bfloat16


def from_behind(value, axis, steps):
    count = lax.axis_size(axis)
    pairs = [(source, (source + steps) % count) for source in range(count)]
    return lax.ppermute(value, axis, pairs)


def gelu_parts(values):
    normal_cdf = 0.5 * (1.0 + lax.erf(values * root_half))
    density = jnp.exp(-0.5 * values * values) * inv_root_tau
    return (values * normal_cdf, normal_cdf + values * density)


def kept_lengths(image_tokens, moved_images):
    present = jnp.sum((image_tokens > 0).astype(jnp.int32), axis=1)
    slot_ids = jnp.arange(image_tokens.shape[1], dtype=jnp.int32)
    kept_mask = slot_ids[None, :] < (present - moved_images)[:, None]
    return jnp.sum(jnp.where(kept_mask, image_tokens, 0), axis=1)


def per_device_any(grad_tokens, hidden_input, output_weight, image_tokens, moved_images):
    dp_count = lax.axis_size("dp")
    dp_index = lax.axis_index("dp")
    tok_rows = grad_tokens.shape[0]
    buffer_rows = hidden_input.shape[0]
    tail_count = buffer_rows - tok_rows
    keep_len = kept_lengths(image_tokens, moved_images)
    own_keep = jnp.sum(jnp.where(jnp.arange(dp_count, dtype=jnp.int32) == dp_index, keep_len, 0))
    positions = jnp.arange(tok_rows, dtype=jnp.int32)[:, None]
    zero_value = jnp.zeros((), BF16)
    kept_rows = jnp.where(positions < own_keep, grad_tokens, zero_value)
    moving = jnp.where(
        positions[tok_rows - tail_count :] >= own_keep,
        grad_tokens[tok_rows - tail_count :],
        zero_value,
    )
    arrived = from_behind(moving, "dp", 1)
    grad_rows = jnp.concatenate([kept_rows, arrived], axis=0)
    bias_grad = lax.psum(jnp.sum(grad_tokens.astype(F32), axis=0), "dp")
    activation, slopes = gelu_parts(hidden_input.astype(F32))
    partials = lax.dot_general(
        grad_rows, output_weight, (((1,), (1,)), ((), ())), preferred_element_type=F32
    )
    grad_hidden = lax.psum_scatter(
        partials.astype(BF16), "tensor", scatter_dimension=1, tiled=True
    ).astype(F32)
    input_grad = (grad_hidden * slopes).astype(BF16)
    full_act = lax.all_gather(activation.astype(BF16), "tensor", axis=1, tiled=True)
    hidden_width = full_act.shape[1]
    rows_each = (hidden_width + 8 * dp_count - 1) // (8 * dp_count) * 8
    padded = jnp.pad(full_act, ((0, 0), (0, rows_each * dp_count - hidden_width)))
    weight_grad = lax.psum_scatter(
        lax.dot_general(
            padded, grad_rows, (((0,), (0,)), ((), ())), preferred_element_type=F32
        ),
        "dp",
        scatter_dimension=0,
        tiled=True,
    )
    return (input_grad, weight_grad, bias_grad)


def kernel(
    n, dpn,
    g_hbm, x_hbm, w_hbm, it_hbm, mv_hbm,
    xg_ref, wg_ref, bg_ref,
    it_ref, mv_ref, w_ref, x_ref, xn, graw, act, act_other, slope, part, sbuf, up_in, dn_in, wsend, wrecv, wmid, bias,
    tsend, trecv,
    plan_sem, w_sem, x_sem, g_sem, core_s, core_r, act_s, act_r, xt_s, xt_r, tail_s, tail_r,
    up0_s, up0_r, dn0_s, dn0_r, up_s, up_r, dn_s, dn_r, pl_s, pl_r, mid_r, bi_s, bi_r,
):
    dp = lax.axis_index("dp")
    z = lax.axis_index("tensor")
    core = lax.rem(dp, 2)
    chip = lax.div(dp, 2)
    partner = dp + 1 - 2 * core
    after = lax.rem(dp + 1, dpn)
    before = lax.rem(dp + dpn - 1, dpn)
    chips = dpn // 2
    tok = g_hbm.shape[0]
    rows, width = x_hbm.shape
    half = width // 2
    tails = rows - tok
    main = tok - tails
    lane = 128
    nk = half // lane
    ptile = width // nk
    late = 2
    early = range(late, nk)
    main_rows = pl.ds(0, main)
    tail_rows = pl.ds(main, tails)
    slot_rows = pl.ds(tok, tails)

    x_copies = [
        pltpu.make_async_copy(x_hbm.at[slot_rows], x_ref.at[slot_rows], x_sem.at[0]),
        pltpu.make_async_copy(x_hbm.at[pl.ds(0, tok)], x_ref.at[pl.ds(0, tok)], x_sem.at[1]),
    ]
    g_copy = pltpu.make_async_copy(g_hbm, graw.at[core], g_sem)
    w_copy = pltpu.make_async_copy(w_hbm, w_ref, w_sem)
    plan_copies = [
        pltpu.make_async_copy(it_hbm, it_ref, plan_sem.at[0]),
        pltpu.make_async_copy(mv_hbm, mv_ref, plan_sem.at[1]),
    ]
    for c in x_copies + plan_copies:
        c.start()
    g_copy.start()
    w_copy.start()

    barrier = pltpu.get_barrier_semaphore()

    def greet(d, t):
        pl.semaphore_signal(barrier, inc=1, device_id=(d, t), device_id_type=MESH)

    for k in range(1, dpn):
        greet(lax.rem(dp + k, dpn), z)

    @pl.when(z > 0)
    def _():
        greet(dp, z - 1)
        greet(partner, z - 1)

    @pl.when(z < n - 1)
    def _():
        greet(dp, z + 1)
        greet(partner, z + 1)

    pl.semaphore_wait(barrier, dpn - 1 + jnp.where(z > 0, 2, 0) + jnp.where(z < n - 1, 2, 0))

    def remote(src, dst, ss, rs, d, t):
        return pltpu.make_async_remote_copy(
            src_ref=src, dst_ref=dst, send_sem=ss, recv_sem=rs, device_id=(d, t), device_id_type=MESH
        )

    x_tail_copy = remote(x_ref.at[slot_rows], xn, xt_s, xt_r, before, z)
    raw_copy = remote(graw.at[core], graw.at[core], core_s, core_r, partner, z)
    x_copies[0].wait()
    x_tail_copy.start()

    for c in plan_copies:
        c.wait()
    images = it_ref[pl.ds(dp, 1), :].astype(F32)
    present = jnp.sum(jnp.where(images > 0, 1.0, 0.0), axis=1, keepdims=True)
    ids = lax.broadcasted_iota(jnp.int32, images.shape, 1).astype(F32)
    keep = jnp.sum(
        jnp.where(ids < present - mv_ref[dp].astype(F32), images, 0.0), axis=1, keepdims=True
    )

    def stays(columns):
        return lax.broadcasted_iota(jnp.int32, (tails, columns), 0).astype(F32) + main < keep

    def pieces(k):
        if k < late:
            return [(k, 0, tok)]
        return [(k, 0, main), (nk + k - late, main, tails)]

    def act_copy(k, p, r0, rn):
        rs = pl.ds(r0, rn)
        return remote(act_other.at[k, rs], act.at[z, k, core, rs], act_s.at[p], act_r.at[p], partner, z)

    def first_copies(k, p, r0, rn, ss, rr, t):
        rs = pl.ds(r0, rn)
        target = act.at[z, k, core, rs]
        return (
            remote(target, target, ss.at[p, 0], rr.at[p, core], dp, t),
            remote(act_other.at[k, rs], target, ss.at[p, 1], rr.at[p, core], partner, t),
        )

    def send_first(k, p, r0, rn):
        @pl.when(z < n - 1)
        def _():
            for c in first_copies(k, p, r0, rn, up0_s, up0_r, z + 1):
                c.start()

        @pl.when(z > 0)
        def _():
            for c in first_copies(k, p, r0, rn, dn0_s, dn0_r, z - 1):
                c.start()

        act_copy(k, p, r0, rn).start()

    step_rows = 64

    def put(to_other, k, rs, a):
        if to_other:
            act_other[k, rs, :] = a
        else:
            act[z, k, core, rs, :] = a

    def normal_cdf(v):
        return 0.5 * (1.0 + lax.erf(v * root_half))

    def columns_of(which, k):
        return pl.ds(pl.multiple_of(which * half + k * lane, lane), lane)

    def gelu_main(k):
        for which, to_other in ((1 - core, True), (core, False)):
            cols = columns_of(which, k)

            def body(i, carry):
                rs = pl.ds(pl.multiple_of(i * step_rows, step_rows), step_rows)
                v = x_ref[rs, cols].astype(F32)
                cdf = normal_cdf(v)
                slope[rs, cols] = cdf
                put(to_other, k, rs, (v * cdf).astype(BF16))
                return carry

            lax.fori_loop(0, main // step_rows, body, 0)

    def gelu_tail(k):
        for which, to_other in ((1 - core, True), (core, False)):
            cols = columns_of(which, k)
            v = x_ref[tail_rows, cols].astype(F32)
            own = normal_cdf(v)
            slope[tail_rows, cols] = own
            u = xn[:, cols].astype(F32)
            other = normal_cdf(u)
            slope[slot_rows, cols] = other
            put(to_other, k, tail_rows, jnp.where(stays(lane), v * own, u * other).astype(BF16))

    x_copies[1].wait()
    for k in early:
        gelu_main(k)
        send_first(k, *pieces(k)[0])
    g_copy.wait()
    raw_copy.start()
    for k in range(late):
        gelu_main(k)
    x_tail_copy.wait_recv()
    for k in range(nk):
        gelu_tail(k)
        send_first(k, *pieces(k)[-1])

    def up_ag(h, k, r):
        return remote(act.at[h, k], act.at[h, k], up_s.at[r - 1, k], up_r.at[r - 1, k], dp, z + 1)

    def dn_ag(h, k, r):
        return remote(act.at[h, k], act.at[h, k], dn_s.at[r - 1, k], dn_r.at[r - 1, k], dp, z - 1)

    def rs_piece(ref, h, c):
        return ref.at[h, :, tail_rows] if c == 0 else ref.at[h, c - 1, main_rows]

    def up_rs(h, c, r):
        return remote(
            rs_piece(sbuf, h, c), rs_piece(up_in, h, c), up_s.at[r - 1, c], up_r.at[r - 1, c], dp, z + 1
        )

    def dn_rs(h, c, r):
        return remote(
            rs_piece(sbuf, h, c), rs_piece(dn_in, h, c), dn_s.at[r - 1, c], dn_r.at[r - 1, c], dp, z - 1
        )

    def add_up(h, c, extra):
        if c == 0:
            total = part[h, :, main:tok, :]
            if extra is not None:
                total = total + extra[h, :, main:tok, :].astype(F32)
            sbuf[h, :, main:tok, :] = total.astype(BF16)
        else:
            total = part[h, c - 1, 0:main, :]
            if extra is not None:
                total = total + extra[h, c - 1, 0:main, :].astype(F32)
            sbuf[h, c - 1, 0:main, :] = total.astype(BF16)

    w_copy.wait()

    def all_h(i, carry):
        h = lax.div(i, nk)
        k = lax.rem(i, nk)
        at = pl.ds(pl.multiple_of(i * ptile, ptile), ptile)
        part[h, k] = lax.dot_general(
            graw[core], w_ref[at, :], (((1,), (1,)), ((), ())), preferred_element_type=F32
        )
        return carry

    lax.fori_loop(0, n * nk, all_h, 0)

    @pl.when(z == 0)
    def _():
        for r in range(1, n):
            for c in range(nk + 1):
                add_up(n - r, c, None)
                up_rs(n - r, c, r).start()

    @pl.when(z == n - 1)
    def _():
        for r in range(1, n):
            for c in range(nk + 1):
                add_up(r - 1, c, None)
                dn_rs(r - 1, c, r).start()

    raw_copy.wait_recv()
    chip_sum = jnp.sum(graw[0].astype(F32), axis=0, keepdims=True) + jnp.sum(
        graw[1].astype(F32), axis=0, keepdims=True
    )
    bias[chip] = jnp.broadcast_to(chip_sum, bias.shape[1:])

    def bias_copy(k):
        return remote(
            bias.at[chip], bias.at[chip], bi_s.at[k], bi_r.at[chip], lax.rem(dp + 2 * k, dpn), z
        )

    for k in range(1, chips):
        bias_copy(k).start()

    piece = lane // 2

    def relation(h):
        return jnp.where(lax.rem(chip, 2) != lax.rem(h, 2), 1, 0) + jnp.where(
            lax.div(chip, 2) != lax.div(h, 2), 2, 0
        )

    along_x = chip + 1 - 2 * lax.rem(chip, 2)
    along_y = lax.rem(chip + 2, chips)

    def owner_copy(h, k, j):
        role = relation(h) - 1
        return remote(
            wsend.at[h, k, j], wrecv.at[role, k, j], pl_s.at[h, k, j], pl_r.at[role, k, j], h * 2 + core, z
        )

    def corner_copy(h, k, j):
        through = along_x if j == 0 else along_y
        return remote(
            wsend.at[h, k, j], wmid.at[1 - j, k], pl_s.at[h, k, j], mid_r.at[1 - j, k], through * 2 + core, z
        )

    def merge(h, k):
        rel = relation(h)
        for role in (1, 2):
            over = 1 if role == 1 else 0

            @pl.when(rel == role)
            def _():
                corner_copy(h, k, over).wait_recv()
                wsend[h, k, over] = (
                    wsend[h, k, over].astype(F32) + wmid[role - 1, k].astype(F32)
                ).astype(BF16)
                owner_copy(h, k, over).start()

    def weight_tile(h, k):
        acc = lax.dot_general(
            act[h, k].reshape(2 * tok, lane),
            graw[...].reshape(2 * tok, graw.shape[2]),
            (((0,), (0,)), ((), ())),
            preferred_element_type=F32,
        )
        rel = relation(h)

        @pl.when(rel == 0)
        def _():
            wg_ref[k * lane : (k + 1) * lane, :] = acc

        @pl.when(rel != 0)
        def _():
            for j in range(2):
                wsend[h, k, j] = acc[j * piece : (j + 1) * piece].astype(BF16)

        @pl.when(rel == 1)
        def _():
            owner_copy(h, k, 0).start()

        @pl.when(rel == 2)
        def _():
            owner_copy(h, k, 1).start()

        @pl.when(rel == 3)
        def _():
            for j in range(2):
                corner_copy(h, k, j).start()

    for k in range(nk):
        for p, r0, rn in pieces(k):
            act_copy(k, p, r0, rn).wait_recv()
        weight_tile(z, k)

    def merge_round(r, k):
        if r == 0:
            merge(z, k)
        else:

            @pl.when(z >= r)
            def _():
                merge(z - r, k)

            @pl.when(z + r <= n - 1)
            def _():
                merge(z + r, k)

    def first_arrivals(h, k, ss, rr):
        for p, r0, rn in pieces(k):
            rs = pl.ds(r0, rn)
            for s in range(2):
                remote(
                    act.at[h, k, s, rs], act.at[h, k, s, rs], ss.at[p, 0], rr.at[p, s], partner, z
                ).wait_recv()

    def finish_slope(k):
        at = slice(k * ptile, (k + 1) * ptile)

        def grow(source, source_rows, target_rows):
            v = source[source_rows, at].astype(F32)
            slope[target_rows, at] += v * (jnp.exp(-0.5 * v * v) * inv_root_tau)

        def body(i, carry):
            rs = pl.ds(pl.multiple_of(i * step_rows, step_rows), step_rows)
            grow(x_ref, rs, rs)
            return carry

        lax.fori_loop(0, tok // step_rows, body, 0)
        grow(xn, pl.ds(0, tails), slot_rows)

    def pass_up(c, r):
        h = n + z - r
        up_rs(h, c, r - 1).wait_recv()
        add_up(h, c, up_in)
        up_rs(h, c, r).start()

    def pass_dn(c, r):
        h = z + r - n
        dn_rs(h, c, r - 1).wait_recv()
        add_up(h, c, dn_in)
        dn_rs(h, c, r).start()

    def last_sum(c):
        index = slice(main, tok) if c == 0 else slice(0, main)
        which = slice(None) if c == 0 else c - 1

        @pl.when(z > 0)
        def _():
            up_rs(z, c, n - 1).wait_recv()
            part[z, which, index, :] += up_in[z, which, index, :].astype(F32)

        @pl.when(z < n - 1)
        def _():
            dn_rs(z, c, n - 1).wait_recv()
            part[z, which, index, :] += dn_in[z, which, index, :].astype(F32)

    tail_copy = remote(tsend, trecv, tail_s, tail_r, after, z)

    def finish_tail():
        last_sum(0)
        zero = jnp.zeros((), F32)
        for k in range(nk):
            at = slice(k * ptile, (k + 1) * ptile)
            total = part[z, k, main:tok, :]
            here = stays(ptile)
            xg_ref[main:tok, at] = jnp.where(here, total * slope[main:tok, at], zero).astype(BF16)
            tsend[:, at] = jnp.where(here, zero, total * slope[tok:rows, at]).astype(BF16)
        tail_copy.start()

    merge_after = {0: [], 1: [0], 2: [1], 3: [], 4: [2], 5: [3, 4]}
    for r in range(1, n):
        for c in range(nk + 1):
            if c < nk:

                @pl.when(z >= r)
                def _():
                    if r == 1:
                        first_arrivals(z - 1, c, up0_s, up0_r)
                    else:
                        up_ag(z - r, c, r - 1).wait_recv()

                    @pl.when(z < n - 1)
                    def _():
                        up_ag(z - r, c, r).start()

                @pl.when(z + r <= n - 1)
                def _():
                    if r == 1:
                        first_arrivals(z + 1, c, dn0_s, dn0_r)
                    else:
                        dn_ag(z + r, c, r - 1).wait_recv()

                    @pl.when(z > 0)
                    def _():
                        dn_ag(z + r, c, r).start()

            if r > 1:
                last = r if c > 0 else r - 1

                @pl.when((z > 0) & (z < last))
                def _():
                    pass_up(c, r)

                @pl.when((z < n - 1) & (z + last > n - 1))
                def _():
                    pass_dn(c, r)

            if c < nk:

                @pl.when(z >= r)
                def _():
                    weight_tile(z - r, c)

                @pl.when(z + r <= n - 1)
                def _():
                    weight_tile(z + r, c)

                merge_round(r - 1, c)
                if r == 1:
                    finish_slope(c)
            if r < n - 1 and c == nk - 2 - r:

                @pl.when(z == r)
                def _():
                    pass_up(0, r + 1)

                @pl.when(z == n - 1 - r)
                def _():
                    pass_dn(0, r + 1)

            if r == n - 1:
                for k in merge_after[c]:
                    merge_round(r, k)
                if c == 1:

                    @pl.when((z == 0) | (z == n - 1))
                    def _():
                        finish_tail()


    @pl.when((z > 0) & (z < n - 1))
    def _():
        finish_tail()

    for k in range(1, chips):
        source = lax.rem(chip + k, chips)
        remote(
            bias.at[source], bias.at[source], bi_s.at[k], bi_r.at[source], lax.rem(dp + 2 * k, dpn), z
        ).wait_recv()
    total = bias[0]
    for k in range(1, chips):
        total = total + bias[k]
    bg_ref[...] = total[0]

    for k in range(nk):
        for j in range(2):
            rs = slice(k * lane + j * piece, k * lane + (j + 1) * piece)
            acc = wg_ref[rs, :]
            for role in range(2):
                remote(
                    wsend.at[along_x, k, j], wrecv.at[role, k, j], pl_s.at[0, k, j], pl_r.at[role, k, j],
                    partner, z,
                ).wait_recv()
                acc = acc + wrecv[role, k, j].astype(F32)
            wg_ref[rs, :] = acc

    for k in range(nk):
        last_sum(k + 1)
        at = slice(k * ptile, (k + 1) * ptile)
        xg_ref[0:main, at] = (part[z, k, 0:main, :] * slope[0:main, at]).astype(BF16)

    tail_copy.wait_recv()
    xg_ref[tok:rows, :] = trecv[...]

    tail_copy.wait_send()
    x_tail_copy.wait_send()
    raw_copy.wait_send()
    for c in range(1, chips):
        bias_copy(c).wait_send()
        h = lax.rem(chip + c, chips)
        for k in range(nk):
            for j in range(2):
                remote(
                    wsend.at[h, k, j], wrecv.at[0, k, j], pl_s.at[h, k, j], pl_r.at[0, k, j], partner, z
                ).wait_send()
    for k in range(nk):
        for p in pieces(k):
            act_copy(k, *p).wait_send()

            @pl.when(z < n - 1)
            def _():
                for c in first_copies(k, *p, up0_s, up0_r, z + 1):
                    c.wait_send()

            @pl.when(z > 0)
            def _():
                for c in first_copies(k, *p, dn0_s, dn0_r, z - 1):
                    c.wait_send()

    for r in range(1, n):

        @pl.when((z < n - 1) & (z >= r))
        def _():
            for k in range(nk):
                up_ag(0, k, r).wait_send()

        @pl.when((z < n - 1) & (z < r))
        def _():
            for c in range(nk + 1):
                up_rs(0, c, r).wait_send()

        @pl.when((z > 0) & (z + r <= n - 1))
        def _():
            for k in range(nk):
                dn_ag(0, k, r).wait_send()

        @pl.when((z > 0) & (z + r > n - 1))
        def _():
            for c in range(nk + 1):
                dn_rs(0, c, r).wait_send()


def writer(a_ref, b_ref, c_ref, a_out, b_out, c_out, sems):
    copies = [
        pltpu.make_async_copy(b_ref, b_out, sems.at[0]),
        pltpu.make_async_copy(a_ref, a_out, sems.at[1]),
        pltpu.make_async_copy(c_ref, c_out, sems.at[2]),
    ]
    for c in copies:
        c.start()
    for c in copies:
        c.wait()


def write_out(*args):
    vmem = pl.BlockSpec(memory_space=pltpu.VMEM)
    hbm = pl.BlockSpec(memory_space=pltpu.HBM)
    return pl.pallas_call(
        writer,
        out_shape=tuple(jax.ShapeDtypeStruct(a.shape, a.dtype) for a in args),
        in_specs=[vmem] * len(args),
        out_specs=tuple([hbm] * len(args)),
        scratch_shapes=[pltpu.SemaphoreType.DMA((len(args),))],
        compiler_params=pltpu.CompilerParams(vmem_limit_bytes=1024 * 1024),
    )(*(pltpu.with_memory_space_constraint(a, pltpu.VMEM) for a in args))


def per_device_fast(n, dpn, *args):
    grad_tokens, hidden_input, output_weight, image_tokens, moved_images = args
    tok, cols = grad_tokens.shape
    rows, width = hidden_input.shape
    half = width // 2
    chips = dpn // 2
    lane = 128
    nk = half // lane
    ptile = width // nk
    npiece = 2 * nk - 2
    dma = pltpu.SemaphoreType.DMA
    vmem = pl.BlockSpec(memory_space=pltpu.VMEM)
    hbm = pl.BlockSpec(memory_space=pltpu.HBM)
    results = pl.pallas_call(
        functools.partial(kernel, n, dpn),
        out_shape=(
            jax.ShapeDtypeStruct((rows, width), BF16),
            jax.ShapeDtypeStruct((half, cols), F32),
            jax.ShapeDtypeStruct((cols,), F32),
        ),
        in_specs=[hbm] * 5,
        out_specs=(vmem, vmem, vmem),
        scratch_shapes=[
            pltpu.VMEM(image_tokens.shape, jnp.int32),
            pltpu.SMEM(moved_images.shape, jnp.int32),
            pltpu.VMEM(output_weight.shape, BF16),
            pltpu.VMEM((rows, width), BF16),
            pltpu.VMEM((rows - tok, width), BF16),
            pltpu.VMEM((2, tok, cols), BF16),
            pltpu.VMEM((n, nk, 2, tok, lane), BF16),
            pltpu.VMEM((nk, tok, lane), BF16),
            pltpu.VMEM((rows, width), F32),
            pltpu.VMEM((n, nk, tok, ptile), F32),
            pltpu.VMEM((n, nk, tok, ptile), BF16),
            pltpu.VMEM((n, nk, tok, ptile), BF16),
            pltpu.VMEM((n, nk, tok, ptile), BF16),
            pltpu.VMEM((chips, nk, 2, lane // 2, cols), BF16),
            pltpu.VMEM((2, nk, 2, lane // 2, cols), BF16),
            pltpu.VMEM((2, nk, lane // 2, cols), BF16),
            pltpu.VMEM((chips, 8, cols), F32),
            pltpu.VMEM((rows - tok, width), BF16),
            pltpu.VMEM((rows - tok, width), BF16),
            dma((2,)),
            dma,
            dma((2,)),
            dma,
            dma,
            dma,
            dma((npiece,)),
            dma((npiece,)),
            dma,
            dma,
            dma,
            dma,
            dma((npiece, 2)),
            dma((npiece, 2)),
            dma((npiece, 2)),
            dma((npiece, 2)),
            dma((n - 1, nk + 1)),
            dma((n - 1, nk + 1)),
            dma((n - 1, nk + 1)),
            dma((n - 1, nk + 1)),
            dma((chips, nk, 2)),
            dma((2, nk, 2)),
            dma((2, nk)),
            dma((chips,)),
            dma((chips,)),
        ],
        compiler_params=pltpu.CompilerParams(
            collective_id=0, has_side_effects=True, vmem_limit_bytes=48 * 1024 * 1024
        ),
    )(*(pltpu.with_memory_space_constraint(a, pltpu.HBM) for a in args))
    return write_out(*results)


def solution(mesh):
    n, dpn = mesh.shape["tensor"], mesh.shape["dp"]
    fast = dpn == 2 * n == 2 * 2 * 2
    return jax.shard_map(
        functools.partial(per_device_fast, n, dpn) if fast else per_device_any,
        mesh=mesh,
        in_specs=(P("dp", "tensor"), P("dp", "tensor"), P(None, "tensor"), P(), P()),
        out_specs=(P("dp", "tensor"), P("dp", "tensor"), P("tensor")),
        check_vma=False,
    )
```

```python
import functools

import jax
import jax.numpy as jnp
from jax import lax
from jax.experimental import pallas as pl
from jax.experimental.pallas import tpu as pltpu
from jax.sharding import PartitionSpec as P

root_half = 0.7071067811865476
inv_root_tau = 0.3989422804014327
MESH = pl.DeviceIdType.MESH
F32 = jnp.float32
BF16 = jnp.bfloat16


def from_behind(value, axis, steps):
    count = lax.axis_size(axis)
    pairs = [(source, (source + steps) % count) for source in range(count)]
    return lax.ppermute(value, axis, pairs)


def gelu_parts(values):
    normal_cdf = 0.5 * (1.0 + lax.erf(values * root_half))
    density = jnp.exp(-0.5 * values * values) * inv_root_tau
    return (values * normal_cdf, normal_cdf + values * density)


def kept_lengths(image_tokens, moved_images):
    present = jnp.sum((image_tokens > 0).astype(jnp.int32), axis=1)
    slot_ids = jnp.arange(image_tokens.shape[1], dtype=jnp.int32)
    kept_mask = slot_ids[None, :] < (present - moved_images)[:, None]
    return jnp.sum(jnp.where(kept_mask, image_tokens, 0), axis=1)


def per_device_any(grad_tokens, hidden_input, output_weight, image_tokens, moved_images):
    dp_count = lax.axis_size("dp")
    dp_index = lax.axis_index("dp")
    tok_rows = grad_tokens.shape[0]
    buffer_rows = hidden_input.shape[0]
    tail_count = buffer_rows - tok_rows
    keep_len = kept_lengths(image_tokens, moved_images)
    own_keep = jnp.sum(jnp.where(jnp.arange(dp_count, dtype=jnp.int32) == dp_index, keep_len, 0))
    positions = jnp.arange(tok_rows, dtype=jnp.int32)[:, None]
    zero_value = jnp.zeros((), BF16)
    kept_rows = jnp.where(positions < own_keep, grad_tokens, zero_value)
    moving = jnp.where(
        positions[tok_rows - tail_count :] >= own_keep,
        grad_tokens[tok_rows - tail_count :],
        zero_value,
    )
    arrived = from_behind(moving, "dp", 1)
    grad_rows = jnp.concatenate([kept_rows, arrived], axis=0)
    bias_grad = lax.psum(jnp.sum(grad_tokens.astype(F32), axis=0), "dp")
    activation, slopes = gelu_parts(hidden_input.astype(F32))
    partials = lax.dot_general(
        grad_rows, output_weight, (((1,), (1,)), ((), ())), preferred_element_type=F32
    )
    grad_hidden = lax.psum_scatter(
        partials.astype(BF16), "tensor", scatter_dimension=1, tiled=True
    ).astype(F32)
    input_grad = (grad_hidden * slopes).astype(BF16)
    full_act = lax.all_gather(activation.astype(BF16), "tensor", axis=1, tiled=True)
    hidden_width = full_act.shape[1]
    rows_each = (hidden_width + 8 * dp_count - 1) // (8 * dp_count) * 8
    padded = jnp.pad(full_act, ((0, 0), (0, rows_each * dp_count - hidden_width)))
    weight_grad = lax.psum_scatter(
        lax.dot_general(
            padded, grad_rows, (((0,), (0,)), ((), ())), preferred_element_type=F32
        ),
        "dp",
        scatter_dimension=0,
        tiled=True,
    )
    return (input_grad, weight_grad, bias_grad)


def kernel(
    n, dpn,
    g_hbm, x_hbm, w_hbm, it_hbm, mv_hbm,
    xg_ref, wg_ref, bg_ref,
    it_ref, mv_ref, w_ref, x_ref, xn, graw, act, act_other, slope, part, sbuf, up_in, dn_in, wsend, wrecv, wmid, bias,
    tsend, trecv,
    plan_sem, w_sem, x_sem, g_sem, core_s, core_r, act_s, act_r, xt_s, xt_r, tail_s, tail_r,
    up0_s, up0_r, dn0_s, dn0_r, up_s, up_r, dn_s, dn_r, pl_s, pl_r, mid_r, bi_s, bi_r,
):
    dp = lax.axis_index("dp")
    z = lax.axis_index("tensor")
    core = lax.rem(dp, 2)
    chip = lax.div(dp, 2)
    partner = dp + 1 - 2 * core
    after = lax.rem(dp + 1, dpn)
    before = lax.rem(dp + dpn - 1, dpn)
    chips = dpn // 2
    tok = g_hbm.shape[0]
    rows, width = x_hbm.shape
    half = width // 2
    tails = rows - tok
    main = tok - tails
    lane = 128
    nk = half // lane
    ptile = width // nk
    late = 2
    early = range(late, nk)
    main_rows = pl.ds(0, main)
    tail_rows = pl.ds(main, tails)
    slot_rows = pl.ds(tok, tails)

    x_copies = [
        pltpu.make_async_copy(x_hbm.at[slot_rows], x_ref.at[slot_rows], x_sem.at[0]),
        pltpu.make_async_copy(x_hbm.at[pl.ds(0, tok)], x_ref.at[pl.ds(0, tok)], x_sem.at[1]),
    ]
    g_copy = pltpu.make_async_copy(g_hbm, graw.at[core], g_sem)
    w_copy = pltpu.make_async_copy(w_hbm, w_ref, w_sem)
    plan_copies = [
        pltpu.make_async_copy(it_hbm, it_ref, plan_sem.at[0]),
        pltpu.make_async_copy(mv_hbm, mv_ref, plan_sem.at[1]),
    ]
    for c in x_copies + plan_copies:
        c.start()
    g_copy.start()
    w_copy.start()

    barrier = pltpu.get_barrier_semaphore()

    def greet(d, t):
        pl.semaphore_signal(barrier, inc=1, device_id=(d, t), device_id_type=MESH)

    for k in range(1, dpn):
        greet(lax.rem(dp + k, dpn), z)

    @pl.when(z > 0)
    def _():
        greet(dp, z - 1)
        greet(partner, z - 1)

    @pl.when(z < n - 1)
    def _():
        greet(dp, z + 1)
        greet(partner, z + 1)

    pl.semaphore_wait(barrier, dpn - 1 + jnp.where(z > 0, 2, 0) + jnp.where(z < n - 1, 2, 0))

    def remote(src, dst, ss, rs, d, t):
        return pltpu.make_async_remote_copy(
            src_ref=src, dst_ref=dst, send_sem=ss, recv_sem=rs, device_id=(d, t), device_id_type=MESH
        )

    x_tail_copy = remote(x_ref.at[slot_rows], xn, xt_s, xt_r, before, z)
    raw_copy = remote(graw.at[core], graw.at[core], core_s, core_r, partner, z)
    x_copies[0].wait()
    x_tail_copy.start()

    for c in plan_copies:
        c.wait()
    images = it_ref[pl.ds(dp, 1), :].astype(F32)
    present = jnp.sum(jnp.where(images > 0, 1.0, 0.0), axis=1, keepdims=True)
    ids = lax.broadcasted_iota(jnp.int32, images.shape, 1).astype(F32)
    keep = jnp.sum(
        jnp.where(ids < present - mv_ref[dp].astype(F32), images, 0.0), axis=1, keepdims=True
    )

    def stays(columns):
        return lax.broadcasted_iota(jnp.int32, (tails, columns), 0).astype(F32) + main < keep

    def pieces(k):
        if k < late:
            return [(k, 0, tok)]
        return [(k, 0, main), (nk + k - late, main, tails)]

    def act_copy(k, p, r0, rn):
        rs = pl.ds(r0, rn)
        return remote(act_other.at[k, rs], act.at[z, k, core, rs], act_s.at[p], act_r.at[p], partner, z)

    def first_copies(k, p, r0, rn, ss, rr, t):
        rs = pl.ds(r0, rn)
        target = act.at[z, k, core, rs]
        return (
            remote(target, target, ss.at[p, 0], rr.at[p, core], dp, t),
            remote(act_other.at[k, rs], target, ss.at[p, 1], rr.at[p, core], partner, t),
        )

    def send_first(k, p, r0, rn):
        @pl.when(z < n - 1)
        def _():
            for c in first_copies(k, p, r0, rn, up0_s, up0_r, z + 1):
                c.start()

        @pl.when(z > 0)
        def _():
            for c in first_copies(k, p, r0, rn, dn0_s, dn0_r, z - 1):
                c.start()

        act_copy(k, p, r0, rn).start()

    step_rows = 64

    def put(to_other, k, rs, a):
        if to_other:
            act_other[k, rs, :] = a
        else:
            act[z, k, core, rs, :] = a

    def normal_cdf(v):
        return 0.5 * (1.0 + lax.erf(v * root_half))

    def columns_of(which, k):
        return pl.ds(pl.multiple_of(which * half + k * lane, lane), lane)

    def gelu_main(k):
        for which, to_other in ((1 - core, True), (core, False)):
            cols = columns_of(which, k)

            def body(i, carry):
                rs = pl.ds(pl.multiple_of(i * step_rows, step_rows), step_rows)
                v = x_ref[rs, cols].astype(F32)
                cdf = normal_cdf(v)
                slope[rs, cols] = cdf
                put(to_other, k, rs, (v * cdf).astype(BF16))
                return carry

            lax.fori_loop(0, main // step_rows, body, 0)

    def gelu_tail(k):
        for which, to_other in ((1 - core, True), (core, False)):
            cols = columns_of(which, k)
            v = x_ref[tail_rows, cols].astype(F32)
            own = normal_cdf(v)
            slope[tail_rows, cols] = own
            u = xn[:, cols].astype(F32)
            other = normal_cdf(u)
            slope[slot_rows, cols] = other
            put(to_other, k, tail_rows, jnp.where(stays(lane), v * own, u * other).astype(BF16))

    x_copies[1].wait()
    for k in early:
        gelu_main(k)
        send_first(k, *pieces(k)[0])
    g_copy.wait()
    raw_copy.start()
    for k in range(late):
        gelu_main(k)
    x_tail_copy.wait_recv()
    for k in range(nk):
        gelu_tail(k)
        send_first(k, *pieces(k)[-1])

    def up_ag(h, k, r):
        return remote(act.at[h, k], act.at[h, k], up_s.at[r - 1, k], up_r.at[r - 1, k], dp, z + 1)

    def dn_ag(h, k, r):
        return remote(act.at[h, k], act.at[h, k], dn_s.at[r - 1, k], dn_r.at[r - 1, k], dp, z - 1)

    def rs_piece(ref, h, c):
        return ref.at[h, :, tail_rows] if c == 0 else ref.at[h, c - 1, main_rows]

    def up_rs(h, c, r):
        return remote(
            rs_piece(sbuf, h, c), rs_piece(up_in, h, c), up_s.at[r - 1, c], up_r.at[r - 1, c], dp, z + 1
        )

    def dn_rs(h, c, r):
        return remote(
            rs_piece(sbuf, h, c), rs_piece(dn_in, h, c), dn_s.at[r - 1, c], dn_r.at[r - 1, c], dp, z - 1
        )

    def add_up(h, c, extra):
        if c == 0:
            total = part[h, :, main:tok, :]
            if extra is not None:
                total = total + extra[h, :, main:tok, :].astype(F32)
            sbuf[h, :, main:tok, :] = total.astype(BF16)
        else:
            total = part[h, c - 1, 0:main, :]
            if extra is not None:
                total = total + extra[h, c - 1, 0:main, :].astype(F32)
            sbuf[h, c - 1, 0:main, :] = total.astype(BF16)

    w_copy.wait()

    def all_h(i, carry):
        h = lax.div(i, nk)
        k = lax.rem(i, nk)
        at = pl.ds(pl.multiple_of(i * ptile, ptile), ptile)
        part[h, k] = lax.dot_general(
            graw[core], w_ref[at, :], (((1,), (1,)), ((), ())), preferred_element_type=F32
        )
        return carry

    lax.fori_loop(0, n * nk, all_h, 0)

    @pl.when(z == 0)
    def _():
        for r in range(1, n):
            for c in range(nk + 1):
                add_up(n - r, c, None)
                up_rs(n - r, c, r).start()

    @pl.when(z == n - 1)
    def _():
        for r in range(1, n):
            for c in range(nk + 1):
                add_up(r - 1, c, None)
                dn_rs(r - 1, c, r).start()

    raw_copy.wait_recv()
    chip_sum = jnp.sum(graw[0].astype(F32), axis=0, keepdims=True) + jnp.sum(
        graw[1].astype(F32), axis=0, keepdims=True
    )
    bias[chip] = jnp.broadcast_to(chip_sum, bias.shape[1:])

    def bias_copy(k):
        return remote(
            bias.at[chip], bias.at[chip], bi_s.at[k], bi_r.at[chip], lax.rem(dp + 2 * k, dpn), z
        )

    for k in range(1, chips):
        bias_copy(k).start()

    piece = lane // 2

    def relation(h):
        return jnp.where(lax.rem(chip, 2) != lax.rem(h, 2), 1, 0) + jnp.where(
            lax.div(chip, 2) != lax.div(h, 2), 2, 0
        )

    along_x = chip + 1 - 2 * lax.rem(chip, 2)
    along_y = lax.rem(chip + 2, chips)

    def owner_copy(h, k, j):
        role = relation(h) - 1
        return remote(
            wsend.at[h, k, j], wrecv.at[role, k, j], pl_s.at[h, k, j], pl_r.at[role, k, j], h * 2 + core, z
        )

    def corner_copy(h, k, j):
        through = along_x if j == 0 else along_y
        return remote(
            wsend.at[h, k, j], wmid.at[1 - j, k], pl_s.at[h, k, j], mid_r.at[1 - j, k], through * 2 + core, z
        )

    def merge(h, k):
        rel = relation(h)
        for role in (1, 2):
            over = 1 if role == 1 else 0

            @pl.when(rel == role)
            def _():
                corner_copy(h, k, over).wait_recv()
                wsend[h, k, over] = (
                    wsend[h, k, over].astype(F32) + wmid[role - 1, k].astype(F32)
                ).astype(BF16)
                owner_copy(h, k, over).start()

    def weight_tile(h, k):
        acc = lax.dot_general(
            act[h, k].reshape(2 * tok, lane),
            graw[...].reshape(2 * tok, graw.shape[2]),
            (((0,), (0,)), ((), ())),
            preferred_element_type=F32,
        )
        rel = relation(h)

        @pl.when(rel == 0)
        def _():
            wg_ref[k * lane : (k + 1) * lane, :] = acc

        @pl.when(rel != 0)
        def _():
            for j in range(2):
                wsend[h, k, j] = acc[j * piece : (j + 1) * piece].astype(BF16)

        @pl.when(rel == 1)
        def _():
            owner_copy(h, k, 0).start()

        @pl.when(rel == 2)
        def _():
            owner_copy(h, k, 1).start()

        @pl.when(rel == 3)
        def _():
            for j in range(2):
                corner_copy(h, k, j).start()

    for k in range(nk):
        for p, r0, rn in pieces(k):
            act_copy(k, p, r0, rn).wait_recv()
        weight_tile(z, k)

    def merge_round(r, k):
        if r == 0:
            merge(z, k)
        else:

            @pl.when(z >= r)
            def _():
                merge(z - r, k)

            @pl.when(z + r <= n - 1)
            def _():
                merge(z + r, k)

    def first_arrivals(h, k, ss, rr):
        for p, r0, rn in pieces(k):
            rs = pl.ds(r0, rn)
            for s in range(2):
                remote(
                    act.at[h, k, s, rs], act.at[h, k, s, rs], ss.at[p, 0], rr.at[p, s], partner, z
                ).wait_recv()

    def finish_slope(k):
        at = slice(k * ptile, (k + 1) * ptile)

        def grow(source, source_rows, target_rows):
            v = source[source_rows, at].astype(F32)
            slope[target_rows, at] += v * (jnp.exp(-0.5 * v * v) * inv_root_tau)

        def body(i, carry):
            rs = pl.ds(pl.multiple_of(i * step_rows, step_rows), step_rows)
            grow(x_ref, rs, rs)
            return carry

        lax.fori_loop(0, tok // step_rows, body, 0)
        grow(xn, pl.ds(0, tails), slot_rows)

    def pass_up(c, r):
        h = n + z - r
        up_rs(h, c, r - 1).wait_recv()
        add_up(h, c, up_in)
        up_rs(h, c, r).start()

    def pass_dn(c, r):
        h = z + r - n
        dn_rs(h, c, r - 1).wait_recv()
        add_up(h, c, dn_in)
        dn_rs(h, c, r).start()

    def last_sum(c):
        index = slice(main, tok) if c == 0 else slice(0, main)
        which = slice(None) if c == 0 else c - 1

        @pl.when(z > 0)
        def _():
            up_rs(z, c, n - 1).wait_recv()
            part[z, which, index, :] += up_in[z, which, index, :].astype(F32)

        @pl.when(z < n - 1)
        def _():
            dn_rs(z, c, n - 1).wait_recv()
            part[z, which, index, :] += dn_in[z, which, index, :].astype(F32)

    tail_copy = remote(tsend, trecv, tail_s, tail_r, after, z)

    def finish_tail():
        last_sum(0)
        zero = jnp.zeros((), F32)
        for k in range(nk):
            at = slice(k * ptile, (k + 1) * ptile)
            total = part[z, k, main:tok, :]
            here = stays(ptile)
            xg_ref[main:tok, at] = jnp.where(here, total * slope[main:tok, at], zero).astype(BF16)
            tsend[:, at] = jnp.where(here, zero, total * slope[tok:rows, at]).astype(BF16)
        tail_copy.start()

    merge_after = {0: [], 1: [], 2: [0], 3: [1], 4: [2], 5: [3, 4]}
    for r in range(1, n):
        for c in range(nk + 1):
            if c < nk:

                @pl.when(z >= r)
                def _():
                    if r == 1:
                        first_arrivals(z - 1, c, up0_s, up0_r)
                    else:
                        up_ag(z - r, c, r - 1).wait_recv()

                    @pl.when(z < n - 1)
                    def _():
                        up_ag(z - r, c, r).start()

                @pl.when(z + r <= n - 1)
                def _():
                    if r == 1:
                        first_arrivals(z + 1, c, dn0_s, dn0_r)
                    else:
                        dn_ag(z + r, c, r - 1).wait_recv()

                    @pl.when(z > 0)
                    def _():
                        dn_ag(z + r, c, r).start()

            if r > 1:
                last = r if c > 0 else r - 1

                @pl.when((z > 0) & (z < last))
                def _():
                    pass_up(c, r)

                @pl.when((z < n - 1) & (z + last > n - 1))
                def _():
                    pass_dn(c, r)

            if c < nk:

                @pl.when(z >= r)
                def _():
                    weight_tile(z - r, c)

                @pl.when(z + r <= n - 1)
                def _():
                    weight_tile(z + r, c)

                merge_round(r - 1, c)
                if r == 1:
                    finish_slope(c)
            if r < n - 1 and c == (4 if r == 1 else 4):

                @pl.when(z == r)
                def _():
                    pass_up(0, r + 1)

                @pl.when(z == n - 1 - r)
                def _():
                    pass_dn(0, r + 1)

            if r == n - 1:
                for k in merge_after[c]:
                    merge_round(r, k)
                if c == 4:

                    @pl.when((z == 0) | (z == n - 1))
                    def _():
                        finish_tail()


    @pl.when((z > 0) & (z < n - 1))
    def _():
        finish_tail()

    for k in range(1, chips):
        source = lax.rem(chip + k, chips)
        remote(
            bias.at[source], bias.at[source], bi_s.at[k], bi_r.at[source], lax.rem(dp + 2 * k, dpn), z
        ).wait_recv()
    total = bias[0]
    for k in range(1, chips):
        total = total + bias[k]
    bg_ref[...] = total[0]

    for k in range(nk):
        for j in range(2):
            rs = slice(k * lane + j * piece, k * lane + (j + 1) * piece)
            acc = wg_ref[rs, :]
            for role in range(2):
                remote(
                    wsend.at[along_x, k, j], wrecv.at[role, k, j], pl_s.at[0, k, j], pl_r.at[role, k, j],
                    partner, z,
                ).wait_recv()
                acc = acc + wrecv[role, k, j].astype(F32)
            wg_ref[rs, :] = acc

    for k in range(nk):
        last_sum(k + 1)
        at = slice(k * ptile, (k + 1) * ptile)
        xg_ref[0:main, at] = (part[z, k, 0:main, :] * slope[0:main, at]).astype(BF16)

    tail_copy.wait_recv()
    xg_ref[tok:rows, :] = trecv[...]

    tail_copy.wait_send()
    x_tail_copy.wait_send()
    raw_copy.wait_send()
    for c in range(1, chips):
        bias_copy(c).wait_send()
        h = lax.rem(chip + c, chips)
        for k in range(nk):
            for j in range(2):
                remote(
                    wsend.at[h, k, j], wrecv.at[0, k, j], pl_s.at[h, k, j], pl_r.at[0, k, j], partner, z
                ).wait_send()
    for k in range(nk):
        for p in pieces(k):
            act_copy(k, *p).wait_send()

            @pl.when(z < n - 1)
            def _():
                for c in first_copies(k, *p, up0_s, up0_r, z + 1):
                    c.wait_send()

            @pl.when(z > 0)
            def _():
                for c in first_copies(k, *p, dn0_s, dn0_r, z - 1):
                    c.wait_send()

    for r in range(1, n):

        @pl.when((z < n - 1) & (z >= r))
        def _():
            for k in range(nk):
                up_ag(0, k, r).wait_send()

        @pl.when((z < n - 1) & (z < r))
        def _():
            for c in range(nk + 1):
                up_rs(0, c, r).wait_send()

        @pl.when((z > 0) & (z + r <= n - 1))
        def _():
            for k in range(nk):
                dn_ag(0, k, r).wait_send()

        @pl.when((z > 0) & (z + r > n - 1))
        def _():
            for c in range(nk + 1):
                dn_rs(0, c, r).wait_send()


def writer(a_ref, b_ref, c_ref, a_out, b_out, c_out, sems):
    copies = [
        pltpu.make_async_copy(b_ref, b_out, sems.at[0]),
        pltpu.make_async_copy(a_ref, a_out, sems.at[1]),
        pltpu.make_async_copy(c_ref, c_out, sems.at[2]),
    ]
    for c in copies:
        c.start()
    for c in copies:
        c.wait()


def write_out(*args):
    vmem = pl.BlockSpec(memory_space=pltpu.VMEM)
    hbm = pl.BlockSpec(memory_space=pltpu.HBM)
    return pl.pallas_call(
        writer,
        out_shape=tuple(jax.ShapeDtypeStruct(a.shape, a.dtype) for a in args),
        in_specs=[vmem] * len(args),
        out_specs=tuple([hbm] * len(args)),
        scratch_shapes=[pltpu.SemaphoreType.DMA((len(args),))],
        compiler_params=pltpu.CompilerParams(vmem_limit_bytes=1024 * 1024),
    )(*(pltpu.with_memory_space_constraint(a, pltpu.VMEM) for a in args))


def per_device_fast(n, dpn, *args):
    grad_tokens, hidden_input, output_weight, image_tokens, moved_images = args
    tok, cols = grad_tokens.shape
    rows, width = hidden_input.shape
    half = width // 2
    chips = dpn // 2
    lane = 128
    nk = half // lane
    ptile = width // nk
    npiece = 2 * nk - 2
    dma = pltpu.SemaphoreType.DMA
    vmem = pl.BlockSpec(memory_space=pltpu.VMEM)
    hbm = pl.BlockSpec(memory_space=pltpu.HBM)
    results = pl.pallas_call(
        functools.partial(kernel, n, dpn),
        out_shape=(
            jax.ShapeDtypeStruct((rows, width), BF16),
            jax.ShapeDtypeStruct((half, cols), F32),
            jax.ShapeDtypeStruct((cols,), F32),
        ),
        in_specs=[hbm] * 5,
        out_specs=(vmem, vmem, vmem),
        scratch_shapes=[
            pltpu.VMEM(image_tokens.shape, jnp.int32),
            pltpu.SMEM(moved_images.shape, jnp.int32),
            pltpu.VMEM(output_weight.shape, BF16),
            pltpu.VMEM((rows, width), BF16),
            pltpu.VMEM((rows - tok, width), BF16),
            pltpu.VMEM((2, tok, cols), BF16),
            pltpu.VMEM((n, nk, 2, tok, lane), BF16),
            pltpu.VMEM((nk, tok, lane), BF16),
            pltpu.VMEM((rows, width), F32),
            pltpu.VMEM((n, nk, tok, ptile), F32),
            pltpu.VMEM((n, nk, tok, ptile), BF16),
            pltpu.VMEM((n, nk, tok, ptile), BF16),
            pltpu.VMEM((n, nk, tok, ptile), BF16),
            pltpu.VMEM((chips, nk, 2, lane // 2, cols), BF16),
            pltpu.VMEM((2, nk, 2, lane // 2, cols), BF16),
            pltpu.VMEM((2, nk, lane // 2, cols), BF16),
            pltpu.VMEM((chips, 8, cols), F32),
            pltpu.VMEM((rows - tok, width), BF16),
            pltpu.VMEM((rows - tok, width), BF16),
            dma((2,)),
            dma,
            dma((2,)),
            dma,
            dma,
            dma,
            dma((npiece,)),
            dma((npiece,)),
            dma,
            dma,
            dma,
            dma,
            dma((npiece, 2)),
            dma((npiece, 2)),
            dma((npiece, 2)),
            dma((npiece, 2)),
            dma((n - 1, nk + 1)),
            dma((n - 1, nk + 1)),
            dma((n - 1, nk + 1)),
            dma((n - 1, nk + 1)),
            dma((chips, nk, 2)),
            dma((2, nk, 2)),
            dma((2, nk)),
            dma((chips,)),
            dma((chips,)),
        ],
        compiler_params=pltpu.CompilerParams(
            collective_id=0, has_side_effects=True, vmem_limit_bytes=48 * 1024 * 1024
        ),
    )(*(pltpu.with_memory_space_constraint(a, pltpu.HBM) for a in args))
    return write_out(*results)


def solution(mesh):
    n, dpn = mesh.shape["tensor"], mesh.shape["dp"]
    fast = dpn == 2 * n == 2 * 2 * 2
    return jax.shard_map(
        functools.partial(per_device_fast, n, dpn) if fast else per_device_any,
        mesh=mesh,
        in_specs=(P("dp", "tensor"), P("dp", "tensor"), P(None, "tensor"), P(), P()),
        out_specs=(P("dp", "tensor"), P("dp", "tensor"), P("tensor")),
        check_vma=False,
    )
```

```python
import functools

import jax
import jax.numpy as jnp
from jax import lax
from jax.experimental import pallas as pl
from jax.experimental.pallas import tpu as pltpu
from jax.sharding import PartitionSpec as P

root_half = 0.7071067811865476
inv_root_tau = 0.3989422804014327
MESH = pl.DeviceIdType.MESH
F32 = jnp.float32
BF16 = jnp.bfloat16


def from_behind(value, axis, steps):
    count = lax.axis_size(axis)
    pairs = [(source, (source + steps) % count) for source in range(count)]
    return lax.ppermute(value, axis, pairs)


def gelu_parts(values):
    normal_cdf = 0.5 * (1.0 + lax.erf(values * root_half))
    density = jnp.exp(-0.5 * values * values) * inv_root_tau
    return (values * normal_cdf, normal_cdf + values * density)


def kept_lengths(image_tokens, moved_images):
    present = jnp.sum((image_tokens > 0).astype(jnp.int32), axis=1)
    slot_ids = jnp.arange(image_tokens.shape[1], dtype=jnp.int32)
    kept_mask = slot_ids[None, :] < (present - moved_images)[:, None]
    return jnp.sum(jnp.where(kept_mask, image_tokens, 0), axis=1)


def per_device_any(grad_tokens, hidden_input, output_weight, image_tokens, moved_images):
    dp_count = lax.axis_size("dp")
    dp_index = lax.axis_index("dp")
    tok_rows = grad_tokens.shape[0]
    buffer_rows = hidden_input.shape[0]
    tail_count = buffer_rows - tok_rows
    keep_len = kept_lengths(image_tokens, moved_images)
    own_keep = jnp.sum(jnp.where(jnp.arange(dp_count, dtype=jnp.int32) == dp_index, keep_len, 0))
    positions = jnp.arange(tok_rows, dtype=jnp.int32)[:, None]
    zero_value = jnp.zeros((), BF16)
    kept_rows = jnp.where(positions < own_keep, grad_tokens, zero_value)
    moving = jnp.where(
        positions[tok_rows - tail_count :] >= own_keep,
        grad_tokens[tok_rows - tail_count :],
        zero_value,
    )
    arrived = from_behind(moving, "dp", 1)
    grad_rows = jnp.concatenate([kept_rows, arrived], axis=0)
    bias_grad = lax.psum(jnp.sum(grad_tokens.astype(F32), axis=0), "dp")
    activation, slopes = gelu_parts(hidden_input.astype(F32))
    partials = lax.dot_general(
        grad_rows, output_weight, (((1,), (1,)), ((), ())), preferred_element_type=F32
    )
    grad_hidden = lax.psum_scatter(
        partials.astype(BF16), "tensor", scatter_dimension=1, tiled=True
    ).astype(F32)
    input_grad = (grad_hidden * slopes).astype(BF16)
    full_act = lax.all_gather(activation.astype(BF16), "tensor", axis=1, tiled=True)
    hidden_width = full_act.shape[1]
    rows_each = (hidden_width + 8 * dp_count - 1) // (8 * dp_count) * 8
    padded = jnp.pad(full_act, ((0, 0), (0, rows_each * dp_count - hidden_width)))
    weight_grad = lax.psum_scatter(
        lax.dot_general(
            padded, grad_rows, (((0,), (0,)), ((), ())), preferred_element_type=F32
        ),
        "dp",
        scatter_dimension=0,
        tiled=True,
    )
    return (input_grad, weight_grad, bias_grad)


def kernel(
    n, dpn,
    g_hbm, x_hbm, w_hbm, it_hbm, mv_hbm,
    xg_ref, wg_ref, bg_ref,
    it_ref, mv_ref, w_ref, x_ref, xn, graw, act, act_other, slope, part, sbuf, up_in, dn_in, wsend, wrecv, wmid, bias,
    tsend, trecv,
    plan_sem, w_sem, x_sem, g_sem, core_s, core_r, act_s, act_r, xt_s, xt_r, tail_s, tail_r,
    up0_s, up0_r, dn0_s, dn0_r, up_s, up_r, dn_s, dn_r, pl_s, pl_r, mid_r, bi_s, bi_r,
):
    dp = lax.axis_index("dp")
    z = lax.axis_index("tensor")
    core = lax.rem(dp, 2)
    chip = lax.div(dp, 2)
    partner = dp + 1 - 2 * core
    after = lax.rem(dp + 1, dpn)
    before = lax.rem(dp + dpn - 1, dpn)
    chips = dpn // 2
    tok = g_hbm.shape[0]
    rows, width = x_hbm.shape
    half = width // 2
    tails = rows - tok
    main = tok - tails
    lane = 128
    nk = half // lane
    ptile = width // nk
    late = 2
    early = range(late, nk)
    main_rows = pl.ds(0, main)
    tail_rows = pl.ds(main, tails)
    slot_rows = pl.ds(tok, tails)

    x_copies = [
        pltpu.make_async_copy(x_hbm.at[slot_rows], x_ref.at[slot_rows], x_sem.at[0]),
        pltpu.make_async_copy(x_hbm.at[pl.ds(0, tok)], x_ref.at[pl.ds(0, tok)], x_sem.at[1]),
    ]
    g_copy = pltpu.make_async_copy(g_hbm, graw.at[core], g_sem)
    w_copy = pltpu.make_async_copy(w_hbm, w_ref, w_sem)
    plan_copies = [
        pltpu.make_async_copy(it_hbm, it_ref, plan_sem.at[0]),
        pltpu.make_async_copy(mv_hbm, mv_ref, plan_sem.at[1]),
    ]
    for c in x_copies + plan_copies:
        c.start()
    g_copy.start()
    w_copy.start()

    barrier = pltpu.get_barrier_semaphore()

    def greet(d, t):
        pl.semaphore_signal(barrier, inc=1, device_id=(d, t), device_id_type=MESH)

    for k in range(1, dpn):
        greet(lax.rem(dp + k, dpn), z)

    @pl.when(z > 0)
    def _():
        greet(dp, z - 1)
        greet(partner, z - 1)

    @pl.when(z < n - 1)
    def _():
        greet(dp, z + 1)
        greet(partner, z + 1)

    pl.semaphore_wait(barrier, dpn - 1 + jnp.where(z > 0, 2, 0) + jnp.where(z < n - 1, 2, 0))

    def remote(src, dst, ss, rs, d, t):
        return pltpu.make_async_remote_copy(
            src_ref=src, dst_ref=dst, send_sem=ss, recv_sem=rs, device_id=(d, t), device_id_type=MESH
        )

    x_tail_copy = remote(x_ref.at[slot_rows], xn, xt_s, xt_r, before, z)
    raw_copy = remote(graw.at[core], graw.at[core], core_s, core_r, partner, z)
    x_copies[0].wait()
    x_tail_copy.start()

    for c in plan_copies:
        c.wait()
    images = it_ref[pl.ds(dp, 1), :].astype(F32)
    present = jnp.sum(jnp.where(images > 0, 1.0, 0.0), axis=1, keepdims=True)
    ids = lax.broadcasted_iota(jnp.int32, images.shape, 1).astype(F32)
    keep = jnp.sum(
        jnp.where(ids < present - mv_ref[dp].astype(F32), images, 0.0), axis=1, keepdims=True
    )

    def stays(columns):
        return lax.broadcasted_iota(jnp.int32, (tails, columns), 0).astype(F32) + main < keep

    def pieces(k):
        if k < late:
            return [(k, 0, tok)]
        return [(k, 0, main), (nk + k - late, main, tails)]

    def act_copy(k, p, r0, rn):
        rs = pl.ds(r0, rn)
        return remote(act_other.at[k, rs], act.at[z, k, core, rs], act_s.at[p], act_r.at[p], partner, z)

    def first_copies(k, p, r0, rn, ss, rr, t):
        rs = pl.ds(r0, rn)
        target = act.at[z, k, core, rs]
        return (
            remote(target, target, ss.at[p, 0], rr.at[p, core], dp, t),
            remote(act_other.at[k, rs], target, ss.at[p, 1], rr.at[p, core], partner, t),
        )

    def send_first(k, p, r0, rn):
        @pl.when(z < n - 1)
        def _():
            for c in first_copies(k, p, r0, rn, up0_s, up0_r, z + 1):
                c.start()

        @pl.when(z > 0)
        def _():
            for c in first_copies(k, p, r0, rn, dn0_s, dn0_r, z - 1):
                c.start()

        act_copy(k, p, r0, rn).start()

    step_rows = 64

    def put(to_other, k, rs, a):
        if to_other:
            act_other[k, rs, :] = a
        else:
            act[z, k, core, rs, :] = a

    def normal_cdf(v):
        return 0.5 * (1.0 + lax.erf(v * root_half))

    def columns_of(which, k):
        return pl.ds(pl.multiple_of(which * half + k * lane, lane), lane)

    def gelu_main(k):
        for which, to_other in ((1 - core, True), (core, False)):
            cols = columns_of(which, k)

            def body(i, carry):
                rs = pl.ds(pl.multiple_of(i * step_rows, step_rows), step_rows)
                v = x_ref[rs, cols].astype(F32)
                cdf = normal_cdf(v)
                slope[rs, cols] = cdf
                put(to_other, k, rs, (v * cdf).astype(BF16))
                return carry

            lax.fori_loop(0, main // step_rows, body, 0)

    def gelu_tail(k):
        for which, to_other in ((1 - core, True), (core, False)):
            cols = columns_of(which, k)
            v = x_ref[tail_rows, cols].astype(F32)
            own = normal_cdf(v)
            slope[tail_rows, cols] = own
            u = xn[:, cols].astype(F32)
            other = normal_cdf(u)
            slope[slot_rows, cols] = other
            put(to_other, k, tail_rows, jnp.where(stays(lane), v * own, u * other).astype(BF16))

    x_copies[1].wait()
    for k in early:
        gelu_main(k)
        send_first(k, *pieces(k)[0])
    g_copy.wait()
    raw_copy.start()
    for k in range(late):
        gelu_main(k)
    x_tail_copy.wait_recv()
    for k in range(nk):
        gelu_tail(k)
        send_first(k, *pieces(k)[-1])

    def up_ag(h, k, r):
        return remote(act.at[h, k], act.at[h, k], up_s.at[r - 1, k], up_r.at[r - 1, k], dp, z + 1)

    def dn_ag(h, k, r):
        return remote(act.at[h, k], act.at[h, k], dn_s.at[r - 1, k], dn_r.at[r - 1, k], dp, z - 1)

    def rs_piece(ref, h, c):
        return ref.at[h, :, tail_rows] if c == 0 else ref.at[h, c - 1, main_rows]

    def up_rs(h, c, r):
        return remote(
            rs_piece(sbuf, h, c), rs_piece(up_in, h, c), up_s.at[r - 1, c], up_r.at[r - 1, c], dp, z + 1
        )

    def dn_rs(h, c, r):
        return remote(
            rs_piece(sbuf, h, c), rs_piece(dn_in, h, c), dn_s.at[r - 1, c], dn_r.at[r - 1, c], dp, z - 1
        )

    def add_up(h, c, extra):
        if c == 0:
            total = part[h, :, main:tok, :]
            if extra is not None:
                total = total + extra[h, :, main:tok, :].astype(F32)
            sbuf[h, :, main:tok, :] = total.astype(BF16)
        else:
            total = part[h, c - 1, 0:main, :]
            if extra is not None:
                total = total + extra[h, c - 1, 0:main, :].astype(F32)
            sbuf[h, c - 1, 0:main, :] = total.astype(BF16)

    w_copy.wait()

    def all_h(i, carry):
        h = lax.div(i, nk)
        k = lax.rem(i, nk)
        at = pl.ds(pl.multiple_of(i * ptile, ptile), ptile)
        part[h, k] = lax.dot_general(
            graw[core], w_ref[at, :], (((1,), (1,)), ((), ())), preferred_element_type=F32
        )
        return carry

    lax.fori_loop(0, n * nk, all_h, 0)

    @pl.when(z == 0)
    def _():
        for r in range(1, n):
            for c in range(nk + 1):
                add_up(n - r, c, None)
                up_rs(n - r, c, r).start()

    @pl.when(z == n - 1)
    def _():
        for r in range(1, n):
            for c in range(nk + 1):
                add_up(r - 1, c, None)
                dn_rs(r - 1, c, r).start()

    raw_copy.wait_recv()
    chip_sum = jnp.sum(graw[0].astype(F32), axis=0, keepdims=True) + jnp.sum(
        graw[1].astype(F32), axis=0, keepdims=True
    )
    bias[chip] = jnp.broadcast_to(chip_sum, bias.shape[1:])

    def bias_copy(k):
        return remote(
            bias.at[chip], bias.at[chip], bi_s.at[k], bi_r.at[chip], lax.rem(dp + 2 * k, dpn), z
        )

    for k in range(1, chips):
        bias_copy(k).start()

    piece = lane // 2

    def relation(h):
        return jnp.where(lax.rem(chip, 2) != lax.rem(h, 2), 1, 0) + jnp.where(
            lax.div(chip, 2) != lax.div(h, 2), 2, 0
        )

    along_x = chip + 1 - 2 * lax.rem(chip, 2)
    along_y = lax.rem(chip + 2, chips)

    def owner_copy(h, k, j):
        role = relation(h) - 1
        return remote(
            wsend.at[h, k, j], wrecv.at[role, k, j], pl_s.at[h, k, j], pl_r.at[role, k, j], h * 2 + core, z
        )

    def corner_copy(h, k, j):
        through = along_x if j == 0 else along_y
        return remote(
            wsend.at[h, k, j], wmid.at[1 - j, k], pl_s.at[h, k, j], mid_r.at[1 - j, k], through * 2 + core, z
        )

    def merge(h, k):
        rel = relation(h)
        for role in (1, 2):
            over = 1 if role == 1 else 0

            @pl.when(rel == role)
            def _():
                corner_copy(h, k, over).wait_recv()
                wsend[h, k, over] = (
                    wsend[h, k, over].astype(F32) + wmid[role - 1, k].astype(F32)
                ).astype(BF16)
                owner_copy(h, k, over).start()

    def weight_tile(h, k):
        acc = lax.dot_general(
            act[h, k].reshape(2 * tok, lane),
            graw[...].reshape(2 * tok, graw.shape[2]),
            (((0,), (0,)), ((), ())),
            preferred_element_type=F32,
        )
        rel = relation(h)

        @pl.when(rel == 0)
        def _():
            wg_ref[k * lane : (k + 1) * lane, :] = acc

        @pl.when(rel != 0)
        def _():
            for j in range(2):
                wsend[h, k, j] = acc[j * piece : (j + 1) * piece].astype(BF16)

        @pl.when(rel == 1)
        def _():
            owner_copy(h, k, 0).start()

        @pl.when(rel == 2)
        def _():
            owner_copy(h, k, 1).start()

        @pl.when(rel == 3)
        def _():
            for j in range(2):
                corner_copy(h, k, j).start()

    for k in range(nk):
        for p, r0, rn in pieces(k):
            act_copy(k, p, r0, rn).wait_recv()
        weight_tile(z, k)

    def merge_round(r, k):
        if r == 0:
            merge(z, k)
        else:

            @pl.when(z >= r)
            def _():
                merge(z - r, k)

            @pl.when(z + r <= n - 1)
            def _():
                merge(z + r, k)

    def first_arrivals(h, k, ss, rr):
        for p, r0, rn in pieces(k):
            rs = pl.ds(r0, rn)
            for s in range(2):
                remote(
                    act.at[h, k, s, rs], act.at[h, k, s, rs], ss.at[p, 0], rr.at[p, s], partner, z
                ).wait_recv()

    def finish_slope(k):
        at = slice(k * ptile, (k + 1) * ptile)

        def grow(source, source_rows, target_rows):
            v = source[source_rows, at].astype(F32)
            slope[target_rows, at] += v * (jnp.exp(-0.5 * v * v) * inv_root_tau)

        def body(i, carry):
            rs = pl.ds(pl.multiple_of(i * step_rows, step_rows), step_rows)
            grow(x_ref, rs, rs)
            return carry

        lax.fori_loop(0, tok // step_rows, body, 0)
        grow(xn, pl.ds(0, tails), slot_rows)

    def pass_up(c, r):
        h = n + z - r
        up_rs(h, c, r - 1).wait_recv()
        add_up(h, c, up_in)
        up_rs(h, c, r).start()

    def pass_dn(c, r):
        h = z + r - n
        dn_rs(h, c, r - 1).wait_recv()
        add_up(h, c, dn_in)
        dn_rs(h, c, r).start()

    def last_sum(c):
        index = slice(main, tok) if c == 0 else slice(0, main)
        which = slice(None) if c == 0 else c - 1

        @pl.when(z > 0)
        def _():
            up_rs(z, c, n - 1).wait_recv()
            part[z, which, index, :] += up_in[z, which, index, :].astype(F32)

        @pl.when(z < n - 1)
        def _():
            dn_rs(z, c, n - 1).wait_recv()
            part[z, which, index, :] += dn_in[z, which, index, :].astype(F32)

    tail_copy = remote(tsend, trecv, tail_s, tail_r, after, z)

    def finish_tail():
        last_sum(0)
        zero = jnp.zeros((), F32)
        for k in range(nk):
            at = slice(k * ptile, (k + 1) * ptile)
            total = part[z, k, main:tok, :]
            here = stays(ptile)
            xg_ref[main:tok, at] = jnp.where(here, total * slope[main:tok, at], zero).astype(BF16)
            tsend[:, at] = jnp.where(here, zero, total * slope[tok:rows, at]).astype(BF16)
        tail_copy.start()

    merge_after = {0: [], 1: [], 2: [0], 3: [1], 4: [], 5: [2, 3, 4]}
    for r in range(1, n):
        for c in range(nk + 1):
            if c < nk:

                @pl.when(z >= r)
                def _():
                    if r == 1:
                        first_arrivals(z - 1, c, up0_s, up0_r)
                    else:
                        up_ag(z - r, c, r - 1).wait_recv()

                    @pl.when(z < n - 1)
                    def _():
                        up_ag(z - r, c, r).start()

                @pl.when(z + r <= n - 1)
                def _():
                    if r == 1:
                        first_arrivals(z + 1, c, dn0_s, dn0_r)
                    else:
                        dn_ag(z + r, c, r - 1).wait_recv()

                    @pl.when(z > 0)
                    def _():
                        dn_ag(z + r, c, r).start()

            if r > 1:
                last = r if c > 0 else r - 1

                @pl.when((z > 0) & (z < last))
                def _():
                    pass_up(c, r)

                @pl.when((z < n - 1) & (z + last > n - 1))
                def _():
                    pass_dn(c, r)

            if c < nk:

                @pl.when(z >= r)
                def _():
                    weight_tile(z - r, c)

                @pl.when(z + r <= n - 1)
                def _():
                    weight_tile(z + r, c)

                merge_round(r - 1, c)
                if r == 1:
                    finish_slope(c)
            if r < n - 1 and c == (4 if r == 1 else 4):

                @pl.when(z == r)
                def _():
                    pass_up(0, r + 1)

                @pl.when(z == n - 1 - r)
                def _():
                    pass_dn(0, r + 1)

            if r == n - 1:
                for k in merge_after[c]:
                    merge_round(r, k)
                if c == 4:

                    @pl.when((z == 0) | (z == n - 1))
                    def _():
                        finish_tail()


    @pl.when((z > 0) & (z < n - 1))
    def _():
        finish_tail()

    for k in range(1, chips):
        source = lax.rem(chip + k, chips)
        remote(
            bias.at[source], bias.at[source], bi_s.at[k], bi_r.at[source], lax.rem(dp + 2 * k, dpn), z
        ).wait_recv()
    total = bias[0]
    for k in range(1, chips):
        total = total + bias[k]
    bg_ref[...] = total[0]

    for k in range(nk):
        for j in range(2):
            rs = slice(k * lane + j * piece, k * lane + (j + 1) * piece)
            acc = wg_ref[rs, :]
            for role in range(2):
                remote(
                    wsend.at[along_x, k, j], wrecv.at[role, k, j], pl_s.at[0, k, j], pl_r.at[role, k, j],
                    partner, z,
                ).wait_recv()
                acc = acc + wrecv[role, k, j].astype(F32)
            wg_ref[rs, :] = acc

    for k in range(nk):
        last_sum(k + 1)
        at = slice(k * ptile, (k + 1) * ptile)
        xg_ref[0:main, at] = (part[z, k, 0:main, :] * slope[0:main, at]).astype(BF16)

    tail_copy.wait_recv()
    xg_ref[tok:rows, :] = trecv[...]

    tail_copy.wait_send()
    x_tail_copy.wait_send()
    raw_copy.wait_send()
    for c in range(1, chips):
        bias_copy(c).wait_send()
        h = lax.rem(chip + c, chips)
        for k in range(nk):
            for j in range(2):
                remote(
                    wsend.at[h, k, j], wrecv.at[0, k, j], pl_s.at[h, k, j], pl_r.at[0, k, j], partner, z
                ).wait_send()
    for k in range(nk):
        for p in pieces(k):
            act_copy(k, *p).wait_send()

            @pl.when(z < n - 1)
            def _():
                for c in first_copies(k, *p, up0_s, up0_r, z + 1):
                    c.wait_send()

            @pl.when(z > 0)
            def _():
                for c in first_copies(k, *p, dn0_s, dn0_r, z - 1):
                    c.wait_send()

    for r in range(1, n):

        @pl.when((z < n - 1) & (z >= r))
        def _():
            for k in range(nk):
                up_ag(0, k, r).wait_send()

        @pl.when((z < n - 1) & (z < r))
        def _():
            for c in range(nk + 1):
                up_rs(0, c, r).wait_send()

        @pl.when((z > 0) & (z + r <= n - 1))
        def _():
            for k in range(nk):
                dn_ag(0, k, r).wait_send()

        @pl.when((z > 0) & (z + r > n - 1))
        def _():
            for c in range(nk + 1):
                dn_rs(0, c, r).wait_send()


def writer(a_ref, b_ref, c_ref, a_out, b_out, c_out, sems):
    copies = [
        pltpu.make_async_copy(b_ref, b_out, sems.at[0]),
        pltpu.make_async_copy(a_ref, a_out, sems.at[1]),
        pltpu.make_async_copy(c_ref, c_out, sems.at[2]),
    ]
    for c in copies:
        c.start()
    for c in copies:
        c.wait()


def write_out(*args):
    vmem = pl.BlockSpec(memory_space=pltpu.VMEM)
    hbm = pl.BlockSpec(memory_space=pltpu.HBM)
    return pl.pallas_call(
        writer,
        out_shape=tuple(jax.ShapeDtypeStruct(a.shape, a.dtype) for a in args),
        in_specs=[vmem] * len(args),
        out_specs=tuple([hbm] * len(args)),
        scratch_shapes=[pltpu.SemaphoreType.DMA((len(args),))],
        compiler_params=pltpu.CompilerParams(vmem_limit_bytes=1024 * 1024),
    )(*(pltpu.with_memory_space_constraint(a, pltpu.VMEM) for a in args))


def per_device_fast(n, dpn, *args):
    grad_tokens, hidden_input, output_weight, image_tokens, moved_images = args
    tok, cols = grad_tokens.shape
    rows, width = hidden_input.shape
    half = width // 2
    chips = dpn // 2
    lane = 128
    nk = half // lane
    ptile = width // nk
    npiece = 2 * nk - 2
    dma = pltpu.SemaphoreType.DMA
    vmem = pl.BlockSpec(memory_space=pltpu.VMEM)
    hbm = pl.BlockSpec(memory_space=pltpu.HBM)
    results = pl.pallas_call(
        functools.partial(kernel, n, dpn),
        out_shape=(
            jax.ShapeDtypeStruct((rows, width), BF16),
            jax.ShapeDtypeStruct((half, cols), F32),
            jax.ShapeDtypeStruct((cols,), F32),
        ),
        in_specs=[hbm] * 5,
        out_specs=(vmem, vmem, vmem),
        scratch_shapes=[
            pltpu.VMEM(image_tokens.shape, jnp.int32),
            pltpu.SMEM(moved_images.shape, jnp.int32),
            pltpu.VMEM(output_weight.shape, BF16),
            pltpu.VMEM((rows, width), BF16),
            pltpu.VMEM((rows - tok, width), BF16),
            pltpu.VMEM((2, tok, cols), BF16),
            pltpu.VMEM((n, nk, 2, tok, lane), BF16),
            pltpu.VMEM((nk, tok, lane), BF16),
            pltpu.VMEM((rows, width), F32),
            pltpu.VMEM((n, nk, tok, ptile), F32),
            pltpu.VMEM((n, nk, tok, ptile), BF16),
            pltpu.VMEM((n, nk, tok, ptile), BF16),
            pltpu.VMEM((n, nk, tok, ptile), BF16),
            pltpu.VMEM((chips, nk, 2, lane // 2, cols), BF16),
            pltpu.VMEM((2, nk, 2, lane // 2, cols), BF16),
            pltpu.VMEM((2, nk, lane // 2, cols), BF16),
            pltpu.VMEM((chips, 8, cols), F32),
            pltpu.VMEM((rows - tok, width), BF16),
            pltpu.VMEM((rows - tok, width), BF16),
            dma((2,)),
            dma,
            dma((2,)),
            dma,
            dma,
            dma,
            dma((npiece,)),
            dma((npiece,)),
            dma,
            dma,
            dma,
            dma,
            dma((npiece, 2)),
            dma((npiece, 2)),
            dma((npiece, 2)),
            dma((npiece, 2)),
            dma((n - 1, nk + 1)),
            dma((n - 1, nk + 1)),
            dma((n - 1, nk + 1)),
            dma((n - 1, nk + 1)),
            dma((chips, nk, 2)),
            dma((2, nk, 2)),
            dma((2, nk)),
            dma((chips,)),
            dma((chips,)),
        ],
        compiler_params=pltpu.CompilerParams(
            collective_id=0, has_side_effects=True, vmem_limit_bytes=48 * 1024 * 1024
        ),
    )(*(pltpu.with_memory_space_constraint(a, pltpu.HBM) for a in args))
    return write_out(*results)


def solution(mesh):
    n, dpn = mesh.shape["tensor"], mesh.shape["dp"]
    fast = dpn == 2 * n == 2 * 2 * 2
    return jax.shard_map(
        functools.partial(per_device_fast, n, dpn) if fast else per_device_any,
        mesh=mesh,
        in_specs=(P("dp", "tensor"), P("dp", "tensor"), P(None, "tensor"), P(), P()),
        out_specs=(P("dp", "tensor"), P("dp", "tensor"), P("tensor")),
        check_vma=False,
    )
```

```python
import functools

import jax
import jax.numpy as jnp
from jax import lax
from jax.experimental import pallas as pl
from jax.experimental.pallas import tpu as pltpu
from jax.sharding import PartitionSpec as P

root_half = 0.7071067811865476
inv_root_tau = 0.3989422804014327
MESH = pl.DeviceIdType.MESH
F32 = jnp.float32
BF16 = jnp.bfloat16


def from_behind(value, axis, steps):
    count = lax.axis_size(axis)
    pairs = [(source, (source + steps) % count) for source in range(count)]
    return lax.ppermute(value, axis, pairs)


def gelu_parts(values):
    normal_cdf = 0.5 * (1.0 + lax.erf(values * root_half))
    density = jnp.exp(-0.5 * values * values) * inv_root_tau
    return (values * normal_cdf, normal_cdf + values * density)


def kept_lengths(image_tokens, moved_images):
    present = jnp.sum((image_tokens > 0).astype(jnp.int32), axis=1)
    slot_ids = jnp.arange(image_tokens.shape[1], dtype=jnp.int32)
    kept_mask = slot_ids[None, :] < (present - moved_images)[:, None]
    return jnp.sum(jnp.where(kept_mask, image_tokens, 0), axis=1)


def per_device_any(grad_tokens, hidden_input, output_weight, image_tokens, moved_images):
    dp_count = lax.axis_size("dp")
    dp_index = lax.axis_index("dp")
    tok_rows = grad_tokens.shape[0]
    buffer_rows = hidden_input.shape[0]
    tail_count = buffer_rows - tok_rows
    keep_len = kept_lengths(image_tokens, moved_images)
    own_keep = jnp.sum(jnp.where(jnp.arange(dp_count, dtype=jnp.int32) == dp_index, keep_len, 0))
    positions = jnp.arange(tok_rows, dtype=jnp.int32)[:, None]
    zero_value = jnp.zeros((), BF16)
    kept_rows = jnp.where(positions < own_keep, grad_tokens, zero_value)
    moving = jnp.where(
        positions[tok_rows - tail_count :] >= own_keep,
        grad_tokens[tok_rows - tail_count :],
        zero_value,
    )
    arrived = from_behind(moving, "dp", 1)
    grad_rows = jnp.concatenate([kept_rows, arrived], axis=0)
    bias_grad = lax.psum(jnp.sum(grad_tokens.astype(F32), axis=0), "dp")
    activation, slopes = gelu_parts(hidden_input.astype(F32))
    partials = lax.dot_general(
        grad_rows, output_weight, (((1,), (1,)), ((), ())), preferred_element_type=F32
    )
    grad_hidden = lax.psum_scatter(
        partials.astype(BF16), "tensor", scatter_dimension=1, tiled=True
    ).astype(F32)
    input_grad = (grad_hidden * slopes).astype(BF16)
    full_act = lax.all_gather(activation.astype(BF16), "tensor", axis=1, tiled=True)
    hidden_width = full_act.shape[1]
    rows_each = (hidden_width + 8 * dp_count - 1) // (8 * dp_count) * 8
    padded = jnp.pad(full_act, ((0, 0), (0, rows_each * dp_count - hidden_width)))
    weight_grad = lax.psum_scatter(
        lax.dot_general(
            padded, grad_rows, (((0,), (0,)), ((), ())), preferred_element_type=F32
        ),
        "dp",
        scatter_dimension=0,
        tiled=True,
    )
    return (input_grad, weight_grad, bias_grad)


def kernel(
    n, dpn,
    g_hbm, x_hbm, w_hbm, it_hbm, mv_hbm,
    xg_ref, wg_ref, bg_ref,
    it_ref, mv_ref, w_ref, x_ref, xn, graw, act, act_other, slope, part, sbuf, up_in, dn_in, wsend, wrecv, wmid, bias,
    tsend, trecv,
    plan_sem, w_sem, x_sem, g_sem, core_s, core_r, act_s, act_r, xt_s, xt_r, tail_s, tail_r,
    up0_s, up0_r, dn0_s, dn0_r, up_s, up_r, dn_s, dn_r, pl_s, pl_r, mid_r, bi_s, bi_r,
):
    dp = lax.axis_index("dp")
    z = lax.axis_index("tensor")
    core = lax.rem(dp, 2)
    chip = lax.div(dp, 2)
    partner = dp + 1 - 2 * core
    after = lax.rem(dp + 1, dpn)
    before = lax.rem(dp + dpn - 1, dpn)
    chips = dpn // 2
    tok = g_hbm.shape[0]
    rows, width = x_hbm.shape
    half = width // 2
    tails = rows - tok
    main = tok - tails
    lane = 128
    nk = half // lane
    ptile = width // nk
    late = 2
    early = range(late, nk)
    main_rows = pl.ds(0, main)
    tail_rows = pl.ds(main, tails)
    slot_rows = pl.ds(tok, tails)

    x_copies = [
        pltpu.make_async_copy(x_hbm.at[slot_rows], x_ref.at[slot_rows], x_sem.at[0]),
        pltpu.make_async_copy(x_hbm.at[pl.ds(0, tok)], x_ref.at[pl.ds(0, tok)], x_sem.at[1]),
    ]
    g_copy = pltpu.make_async_copy(g_hbm, graw.at[core], g_sem)
    w_copy = pltpu.make_async_copy(w_hbm, w_ref, w_sem)
    plan_copies = [
        pltpu.make_async_copy(it_hbm, it_ref, plan_sem.at[0]),
        pltpu.make_async_copy(mv_hbm, mv_ref, plan_sem.at[1]),
    ]
    for c in x_copies + plan_copies:
        c.start()
    g_copy.start()
    w_copy.start()

    barrier = pltpu.get_barrier_semaphore()

    def greet(d, t):
        pl.semaphore_signal(barrier, inc=1, device_id=(d, t), device_id_type=MESH)

    for k in range(1, dpn):
        greet(lax.rem(dp + k, dpn), z)

    @pl.when(z > 0)
    def _():
        greet(dp, z - 1)
        greet(partner, z - 1)

    @pl.when(z < n - 1)
    def _():
        greet(dp, z + 1)
        greet(partner, z + 1)


    def remote(src, dst, ss, rs, d, t):
        return pltpu.make_async_remote_copy(
            src_ref=src, dst_ref=dst, send_sem=ss, recv_sem=rs, device_id=(d, t), device_id_type=MESH
        )

    x_tail_copy = remote(x_ref.at[slot_rows], xn, xt_s, xt_r, before, z)
    raw_copy = remote(graw.at[core], graw.at[core], core_s, core_r, partner, z)

    for c in plan_copies:
        c.wait()
    images = it_ref[pl.ds(dp, 1), :].astype(F32)
    present = jnp.sum(jnp.where(images > 0, 1.0, 0.0), axis=1, keepdims=True)
    ids = lax.broadcasted_iota(jnp.int32, images.shape, 1).astype(F32)
    keep = jnp.sum(
        jnp.where(ids < present - mv_ref[dp].astype(F32), images, 0.0), axis=1, keepdims=True
    )

    def stays(columns):
        return lax.broadcasted_iota(jnp.int32, (tails, columns), 0).astype(F32) + main < keep

    def pieces(k):
        if k < late:
            return [(k, 0, tok)]
        return [(k, 0, main), (nk + k - late, main, tails)]

    def act_copy(k, p, r0, rn):
        rs = pl.ds(r0, rn)
        return remote(act_other.at[k, rs], act.at[z, k, core, rs], act_s.at[p], act_r.at[p], partner, z)

    def first_copies(k, p, r0, rn, ss, rr, t):
        rs = pl.ds(r0, rn)
        target = act.at[z, k, core, rs]
        return (
            remote(target, target, ss.at[p, 0], rr.at[p, core], dp, t),
            remote(act_other.at[k, rs], target, ss.at[p, 1], rr.at[p, core], partner, t),
        )

    def send_first(k, p, r0, rn):
        @pl.when(z < n - 1)
        def _():
            for c in first_copies(k, p, r0, rn, up0_s, up0_r, z + 1):
                c.start()

        @pl.when(z > 0)
        def _():
            for c in first_copies(k, p, r0, rn, dn0_s, dn0_r, z - 1):
                c.start()

        act_copy(k, p, r0, rn).start()

    step_rows = 64

    def put(to_other, k, rs, a):
        if to_other:
            act_other[k, rs, :] = a
        else:
            act[z, k, core, rs, :] = a

    def normal_cdf(v):
        return 0.5 * (1.0 + lax.erf(v * root_half))

    def columns_of(which, k):
        return pl.ds(pl.multiple_of(which * half + k * lane, lane), lane)

    def gelu_main(k):
        for which, to_other in ((1 - core, True), (core, False)):
            cols = columns_of(which, k)

            def body(i, carry):
                rs = pl.ds(pl.multiple_of(i * step_rows, step_rows), step_rows)
                v = x_ref[rs, cols].astype(F32)
                cdf = normal_cdf(v)
                slope[rs, cols] = cdf
                put(to_other, k, rs, (v * cdf).astype(BF16))
                return carry

            lax.fori_loop(0, main // step_rows, body, 0)

    def gelu_tail(k):
        for which, to_other in ((1 - core, True), (core, False)):
            cols = columns_of(which, k)
            v = x_ref[tail_rows, cols].astype(F32)
            own = normal_cdf(v)
            slope[tail_rows, cols] = own
            u = xn[:, cols].astype(F32)
            other = normal_cdf(u)
            slope[slot_rows, cols] = other
            put(to_other, k, tail_rows, jnp.where(stays(lane), v * own, u * other).astype(BF16))

    x_copies[1].wait()
    gelu_main(late)
    pl.semaphore_wait(barrier, dpn - 1 + jnp.where(z > 0, 2, 0) + jnp.where(z < n - 1, 2, 0))
    x_copies[0].wait()
    x_tail_copy.start()
    for k in early:
        if k > late:
            gelu_main(k)
        send_first(k, *pieces(k)[0])
    g_copy.wait()
    raw_copy.start()
    for k in range(late):
        gelu_main(k)
    x_tail_copy.wait_recv()
    for k in range(nk):
        gelu_tail(k)
        send_first(k, *pieces(k)[-1])

    def up_ag(h, k, r):
        return remote(act.at[h, k], act.at[h, k], up_s.at[r - 1, k], up_r.at[r - 1, k], dp, z + 1)

    def dn_ag(h, k, r):
        return remote(act.at[h, k], act.at[h, k], dn_s.at[r - 1, k], dn_r.at[r - 1, k], dp, z - 1)

    def rs_piece(ref, h, c):
        return ref.at[h, :, tail_rows] if c == 0 else ref.at[h, c - 1, main_rows]

    def up_rs(h, c, r):
        return remote(
            rs_piece(sbuf, h, c), rs_piece(up_in, h, c), up_s.at[r - 1, c], up_r.at[r - 1, c], dp, z + 1
        )

    def dn_rs(h, c, r):
        return remote(
            rs_piece(sbuf, h, c), rs_piece(dn_in, h, c), dn_s.at[r - 1, c], dn_r.at[r - 1, c], dp, z - 1
        )

    def add_up(h, c, extra):
        if c == 0:
            total = part[h, :, main:tok, :]
            if extra is not None:
                total = total + extra[h, :, main:tok, :].astype(F32)
            sbuf[h, :, main:tok, :] = total.astype(BF16)
        else:
            total = part[h, c - 1, 0:main, :]
            if extra is not None:
                total = total + extra[h, c - 1, 0:main, :].astype(F32)
            sbuf[h, c - 1, 0:main, :] = total.astype(BF16)

    w_copy.wait()

    def all_h(i, carry):
        h = lax.div(i, nk)
        k = lax.rem(i, nk)
        at = pl.ds(pl.multiple_of(i * ptile, ptile), ptile)
        part[h, k] = lax.dot_general(
            graw[core], w_ref[at, :], (((1,), (1,)), ((), ())), preferred_element_type=F32
        )
        return carry

    lax.fori_loop(0, n * nk, all_h, 0)

    @pl.when(z == 0)
    def _():
        for r in range(1, n):
            for c in range(nk + 1):
                add_up(n - r, c, None)
                up_rs(n - r, c, r).start()

    @pl.when(z == n - 1)
    def _():
        for r in range(1, n):
            for c in range(nk + 1):
                add_up(r - 1, c, None)
                dn_rs(r - 1, c, r).start()

    raw_copy.wait_recv()
    chip_sum = jnp.sum(graw[0].astype(F32), axis=0, keepdims=True) + jnp.sum(
        graw[1].astype(F32), axis=0, keepdims=True
    )
    bias[chip] = jnp.broadcast_to(chip_sum, bias.shape[1:])

    def bias_copy(k):
        return remote(
            bias.at[chip], bias.at[chip], bi_s.at[k], bi_r.at[chip], lax.rem(dp + 2 * k, dpn), z
        )

    for k in range(1, chips):
        bias_copy(k).start()

    piece = lane // 2

    def relation(h):
        return jnp.where(lax.rem(chip, 2) != lax.rem(h, 2), 1, 0) + jnp.where(
            lax.div(chip, 2) != lax.div(h, 2), 2, 0
        )

    along_x = chip + 1 - 2 * lax.rem(chip, 2)
    along_y = lax.rem(chip + 2, chips)

    def owner_copy(h, k, j):
        role = relation(h) - 1
        return remote(
            wsend.at[h, k, j], wrecv.at[role, k, j], pl_s.at[h, k, j], pl_r.at[role, k, j], h * 2 + core, z
        )

    def corner_copy(h, k, j):
        through = along_x if j == 0 else along_y
        return remote(
            wsend.at[h, k, j], wmid.at[1 - j, k], pl_s.at[h, k, j], mid_r.at[1 - j, k], through * 2 + core, z
        )

    def merge(h, k):
        rel = relation(h)
        for role in (1, 2):
            over = 1 if role == 1 else 0

            @pl.when(rel == role)
            def _():
                corner_copy(h, k, over).wait_recv()
                wsend[h, k, over] = (
                    wsend[h, k, over].astype(F32) + wmid[role - 1, k].astype(F32)
                ).astype(BF16)
                owner_copy(h, k, over).start()

    def weight_tile(h, k):
        acc = lax.dot_general(
            act[h, k].reshape(2 * tok, lane),
            graw[...].reshape(2 * tok, graw.shape[2]),
            (((0,), (0,)), ((), ())),
            preferred_element_type=F32,
        )
        rel = relation(h)

        @pl.when(rel == 0)
        def _():
            wg_ref[k * lane : (k + 1) * lane, :] = acc

        @pl.when(rel != 0)
        def _():
            for j in range(2):
                wsend[h, k, j] = acc[j * piece : (j + 1) * piece].astype(BF16)

        @pl.when(rel == 1)
        def _():
            owner_copy(h, k, 0).start()

        @pl.when(rel == 2)
        def _():
            owner_copy(h, k, 1).start()

        @pl.when(rel == 3)
        def _():
            for j in range(2):
                corner_copy(h, k, j).start()

    for k in range(nk):
        for p, r0, rn in pieces(k):
            act_copy(k, p, r0, rn).wait_recv()
        weight_tile(z, k)

    def merge_round(r, k):
        if r == 0:
            merge(z, k)
        else:

            @pl.when(z >= r)
            def _():
                merge(z - r, k)

            @pl.when(z + r <= n - 1)
            def _():
                merge(z + r, k)

    def first_arrivals(h, k, ss, rr):
        for p, r0, rn in pieces(k):
            rs = pl.ds(r0, rn)
            for s in range(2):
                remote(
                    act.at[h, k, s, rs], act.at[h, k, s, rs], ss.at[p, 0], rr.at[p, s], partner, z
                ).wait_recv()

    def finish_slope(k):
        at = slice(k * ptile, (k + 1) * ptile)

        def grow(source, source_rows, target_rows):
            v = source[source_rows, at].astype(F32)
            slope[target_rows, at] += v * (jnp.exp(-0.5 * v * v) * inv_root_tau)

        def body(i, carry):
            rs = pl.ds(pl.multiple_of(i * step_rows, step_rows), step_rows)
            grow(x_ref, rs, rs)
            return carry

        lax.fori_loop(0, tok // step_rows, body, 0)
        grow(xn, pl.ds(0, tails), slot_rows)

    def pass_up(c, r):
        h = n + z - r
        up_rs(h, c, r - 1).wait_recv()
        add_up(h, c, up_in)
        up_rs(h, c, r).start()

    def pass_dn(c, r):
        h = z + r - n
        dn_rs(h, c, r - 1).wait_recv()
        add_up(h, c, dn_in)
        dn_rs(h, c, r).start()

    def last_sum(c):
        index = slice(main, tok) if c == 0 else slice(0, main)
        which = slice(None) if c == 0 else c - 1

        @pl.when(z > 0)
        def _():
            up_rs(z, c, n - 1).wait_recv()
            part[z, which, index, :] += up_in[z, which, index, :].astype(F32)

        @pl.when(z < n - 1)
        def _():
            dn_rs(z, c, n - 1).wait_recv()
            part[z, which, index, :] += dn_in[z, which, index, :].astype(F32)

    tail_copy = remote(tsend, trecv, tail_s, tail_r, after, z)

    def finish_tail():
        last_sum(0)
        zero = jnp.zeros((), F32)
        for k in range(nk):
            at = slice(k * ptile, (k + 1) * ptile)
            total = part[z, k, main:tok, :]
            here = stays(ptile)
            xg_ref[main:tok, at] = jnp.where(here, total * slope[main:tok, at], zero).astype(BF16)
            tsend[:, at] = jnp.where(here, zero, total * slope[tok:rows, at]).astype(BF16)
        tail_copy.start()

    merge_after = {0: [], 1: [], 2: [0], 3: [1], 4: [], 5: [2, 3, 4]}
    for r in range(1, n):
        for c in range(nk + 1):
            if c < nk:

                @pl.when(z >= r)
                def _():
                    if r == 1:
                        first_arrivals(z - 1, c, up0_s, up0_r)
                    else:
                        up_ag(z - r, c, r - 1).wait_recv()

                    @pl.when(z < n - 1)
                    def _():
                        up_ag(z - r, c, r).start()

                @pl.when(z + r <= n - 1)
                def _():
                    if r == 1:
                        first_arrivals(z + 1, c, dn0_s, dn0_r)
                    else:
                        dn_ag(z + r, c, r - 1).wait_recv()

                    @pl.when(z > 0)
                    def _():
                        dn_ag(z + r, c, r).start()

            if r > 1:
                last = r if c > 0 else r - 1

                @pl.when((z > 0) & (z < last))
                def _():
                    pass_up(c, r)

                @pl.when((z < n - 1) & (z + last > n - 1))
                def _():
                    pass_dn(c, r)

            if c < nk:

                @pl.when(z >= r)
                def _():
                    weight_tile(z - r, c)

                @pl.when(z + r <= n - 1)
                def _():
                    weight_tile(z + r, c)

                merge_round(r - 1, c)
                if r == 1:
                    finish_slope(c)
            if r < n - 1 and c == (4 if r == 1 else 4):

                @pl.when(z == r)
                def _():
                    pass_up(0, r + 1)

                @pl.when(z == n - 1 - r)
                def _():
                    pass_dn(0, r + 1)

            if r == n - 1:
                for k in merge_after[c]:
                    merge_round(r, k)
                if c == 4:

                    @pl.when((z == 0) | (z == n - 1))
                    def _():
                        finish_tail()


    @pl.when((z > 0) & (z < n - 1))
    def _():
        finish_tail()

    for k in range(1, chips):
        source = lax.rem(chip + k, chips)
        remote(
            bias.at[source], bias.at[source], bi_s.at[k], bi_r.at[source], lax.rem(dp + 2 * k, dpn), z
        ).wait_recv()
    total = bias[0]
    for k in range(1, chips):
        total = total + bias[k]
    bg_ref[...] = total[0]

    def keep_tile(k):
        for j in range(2):
            rs = slice(k * lane + j * piece, k * lane + (j + 1) * piece)
            acc = wg_ref[rs, :]
            for role in range(2):
                remote(
                    wsend.at[along_x, k, j], wrecv.at[role, k, j], pl_s.at[0, k, j], pl_r.at[role, k, j],
                    partner, z,
                ).wait_recv()
                acc = acc + wrecv[role, k, j].astype(F32)
            wg_ref[rs, :] = acc

    for k in range(nk - 2):
        keep_tile(k)

    for k in range(nk):
        last_sum(k + 1)
        at = slice(k * ptile, (k + 1) * ptile)
        xg_ref[0:main, at] = (part[z, k, 0:main, :] * slope[0:main, at]).astype(BF16)

    for k in range(nk - 2, nk):
        keep_tile(k)

    tail_copy.wait_recv()
    xg_ref[tok:rows, :] = trecv[...]

    tail_copy.wait_send()
    x_tail_copy.wait_send()
    raw_copy.wait_send()
    for c in range(1, chips):
        bias_copy(c).wait_send()
        h = lax.rem(chip + c, chips)
        for k in range(nk):
            for j in range(2):
                remote(
                    wsend.at[h, k, j], wrecv.at[0, k, j], pl_s.at[h, k, j], pl_r.at[0, k, j], partner, z
                ).wait_send()
    for k in range(nk):
        for p in pieces(k):
            act_copy(k, *p).wait_send()

            @pl.when(z < n - 1)
            def _():
                for c in first_copies(k, *p, up0_s, up0_r, z + 1):
                    c.wait_send()

            @pl.when(z > 0)
            def _():
                for c in first_copies(k, *p, dn0_s, dn0_r, z - 1):
                    c.wait_send()

    for r in range(1, n):

        @pl.when((z < n - 1) & (z >= r))
        def _():
            for k in range(nk):
                up_ag(0, k, r).wait_send()

        @pl.when((z < n - 1) & (z < r))
        def _():
            for c in range(nk + 1):
                up_rs(0, c, r).wait_send()

        @pl.when((z > 0) & (z + r <= n - 1))
        def _():
            for k in range(nk):
                dn_ag(0, k, r).wait_send()

        @pl.when((z > 0) & (z + r > n - 1))
        def _():
            for c in range(nk + 1):
                dn_rs(0, c, r).wait_send()


def writer(a_ref, b_ref, c_ref, a_out, b_out, c_out, sems):
    copies = [
        pltpu.make_async_copy(b_ref, b_out, sems.at[0]),
        pltpu.make_async_copy(a_ref, a_out, sems.at[1]),
        pltpu.make_async_copy(c_ref, c_out, sems.at[2]),
    ]
    for c in copies:
        c.start()
    for c in copies:
        c.wait()


def write_out(*args):
    vmem = pl.BlockSpec(memory_space=pltpu.VMEM)
    hbm = pl.BlockSpec(memory_space=pltpu.HBM)
    return pl.pallas_call(
        writer,
        out_shape=tuple(jax.ShapeDtypeStruct(a.shape, a.dtype) for a in args),
        in_specs=[vmem] * len(args),
        out_specs=tuple([hbm] * len(args)),
        scratch_shapes=[pltpu.SemaphoreType.DMA((len(args),))],
        compiler_params=pltpu.CompilerParams(vmem_limit_bytes=1024 * 1024),
    )(*(pltpu.with_memory_space_constraint(a, pltpu.VMEM) for a in args))


def per_device_fast(n, dpn, *args):
    grad_tokens, hidden_input, output_weight, image_tokens, moved_images = args
    tok, cols = grad_tokens.shape
    rows, width = hidden_input.shape
    half = width // 2
    chips = dpn // 2
    lane = 128
    nk = half // lane
    ptile = width // nk
    npiece = 2 * nk - 2
    dma = pltpu.SemaphoreType.DMA
    vmem = pl.BlockSpec(memory_space=pltpu.VMEM)
    hbm = pl.BlockSpec(memory_space=pltpu.HBM)
    results = pl.pallas_call(
        functools.partial(kernel, n, dpn),
        out_shape=(
            jax.ShapeDtypeStruct((rows, width), BF16),
            jax.ShapeDtypeStruct((half, cols), F32),
            jax.ShapeDtypeStruct((cols,), F32),
        ),
        in_specs=[hbm] * 5,
        out_specs=(vmem, vmem, vmem),
        scratch_shapes=[
            pltpu.VMEM(image_tokens.shape, jnp.int32),
            pltpu.SMEM(moved_images.shape, jnp.int32),
            pltpu.VMEM(output_weight.shape, BF16),
            pltpu.VMEM((rows, width), BF16),
            pltpu.VMEM((rows - tok, width), BF16),
            pltpu.VMEM((2, tok, cols), BF16),
            pltpu.VMEM((n, nk, 2, tok, lane), BF16),
            pltpu.VMEM((nk, tok, lane), BF16),
            pltpu.VMEM((rows, width), F32),
            pltpu.VMEM((n, nk, tok, ptile), F32),
            pltpu.VMEM((n, nk, tok, ptile), BF16),
            pltpu.VMEM((n, nk, tok, ptile), BF16),
            pltpu.VMEM((n, nk, tok, ptile), BF16),
            pltpu.VMEM((chips, nk, 2, lane // 2, cols), BF16),
            pltpu.VMEM((2, nk, 2, lane // 2, cols), BF16),
            pltpu.VMEM((2, nk, lane // 2, cols), BF16),
            pltpu.VMEM((chips, 8, cols), F32),
            pltpu.VMEM((rows - tok, width), BF16),
            pltpu.VMEM((rows - tok, width), BF16),
            dma((2,)),
            dma,
            dma((2,)),
            dma,
            dma,
            dma,
            dma((npiece,)),
            dma((npiece,)),
            dma,
            dma,
            dma,
            dma,
            dma((npiece, 2)),
            dma((npiece, 2)),
            dma((npiece, 2)),
            dma((npiece, 2)),
            dma((n - 1, nk + 1)),
            dma((n - 1, nk + 1)),
            dma((n - 1, nk + 1)),
            dma((n - 1, nk + 1)),
            dma((chips, nk, 2)),
            dma((2, nk, 2)),
            dma((2, nk)),
            dma((chips,)),
            dma((chips,)),
        ],
        compiler_params=pltpu.CompilerParams(
            collective_id=0, has_side_effects=True, vmem_limit_bytes=48 * 1024 * 1024
        ),
    )(*(pltpu.with_memory_space_constraint(a, pltpu.HBM) for a in args))
    return write_out(*results)


def solution(mesh):
    n, dpn = mesh.shape["tensor"], mesh.shape["dp"]
    fast = dpn == 2 * n == 2 * 2 * 2
    return jax.shard_map(
        functools.partial(per_device_fast, n, dpn) if fast else per_device_any,
        mesh=mesh,
        in_specs=(P("dp", "tensor"), P("dp", "tensor"), P(None, "tensor"), P(), P()),
        out_specs=(P("dp", "tensor"), P("dp", "tensor"), P("tensor")),
        check_vma=False,
    )
```
